32 devices in a mesh: seq: 4 (over z), tp: 8 (over y, x, core).
Axes of the slice: x: 2, y: 2, z: 4, core: 2. Of those that a mesh axis runs over, the one named last changes fastest.
Arguments:
- tokens: bfloat16 [2048, 4096], P('seq'), may hold values from -80 to 80
- norm_gain: float32 [4096], replicated, may hold values from 0.1 to 1.9
- query_weight: bfloat16 [4096, 4096], P(None, 'tp'), may hold values from -1 to 1
- key_weight: bfloat16 [4096, 1024], P(None, 'tp'), may hold values from -8 to 8
- value_weight: bfloat16 [4096, 1024], P(None, 'tp'), may hold values from -0.09375 to 0.09375
- out_weight: bfloat16 [4096, 4096], P(None, 'tp'), may hold values from -1 to 1
- segments: int32 [2048], replicated, may hold values from 0 to 2, never falling along the last dimension, each value on 1 to 1024 neighbouring positions
Outputs:
- attn_out: bfloat16 [2048, 4096], P('seq', 'tp')
The draws below stay inside these ranges and needn't reach their ends.
All inputs are finite; a program needn't handle non-finite values.
Results may differ from the reference program's by a relative error of at most 0.013.
The reference program's roundings to bfloat16 on the way (of `normed`, `queries`, `keys`, `values`, `probabilities` and `attended`) count: a program that leaves them out, or rounds other values in their place, can miss the bound.
Values may be sent and summed in bfloat16 or wider, within the bound.
No kernel may reach another device: no remote copies, remote signals or barrier semaphores. Data moves between devices by JAX's collectives and lax.ppermute only.
A program may use at most 128 MiB of HBM per device.

```python
import math
import jax
import jax.numpy as jnp
import numpy as np
from jax import lax

D = 4096
HEADS = 32
KV_HEADS = 8
HEAD_DIM = 128
WINDOW = 4096
TOK_DEV = 512
TOKENS = 2048
HALO = 3
N_SEQ = 4


def shared_query(key):
    return jax.random.normal(jax.random.fold_in(key, 11), (D, HEADS * HEAD_DIM), jnp.float32) / math.sqrt(D)


def draw_query_weight(key, part):
    return jnp.clip(shared_query(key), -1.0, 1.0).astype(jnp.bfloat16)


def draw_key_weight(key, part):
    base = jax.random.normal(jax.random.fold_in(key, 13), (D, KV_HEADS * HEAD_DIM), jnp.float32) / math.sqrt(D)
    return jnp.clip(base, -8.0, 8.0).astype(jnp.bfloat16)


def draw_tokens(key, part):
    base = jax.random.normal(jax.random.fold_in(key, 17), (TOKENS, D), jnp.float32)
    base = jnp.clip(base, -6.0, 6.0)
    return base.astype(jnp.bfloat16)


def block_levels(rng, extent, split, low, largest):
    def one(position, blocks):
        steps = jax.random.uniform(jax.random.fold_in(jax.random.fold_in(rng, 6), position), (blocks,), jnp.float32, low / len(split), largest / len(split))
        return jnp.repeat(jnp.exp(steps), extent[position] // blocks).reshape((-1,) + (1,) * (len(extent) - position - 1))

    factor_of = one(*split[0])
    for cut in split[1:]:
        factor_of = factor_of * one(*cut)
    return factor_of


def split_up(number_of, total, most, lean):
    weights = [(1 << 20) // math.isqrt(rank ** lean) + 1 for rank in range(2, number_of + 1)]
    surplus, counts = total - most - (number_of - 1), [1] * (number_of - 1)
    while surplus > 0:
        candidates = [i for i in range(number_of - 1) if counts[i] < most]
        mass, budget = sum([weights[i] for i in candidates]), surplus
        for i in candidates:
            extra = min(most - counts[i], max(1, budget * weights[i] // mass), surplus)
            counts[i] = counts[i] + extra
            surplus = surplus - extra
    return np.array([most] + counts)


def ragged_sizes(stream_key, count, total, most, skew):
    if count == 2:
        one = jax.random.randint(stream_key, (), max(1, total - most), min(most, total - 1) + 1)
        return jnp.stack([one, total - one])
    sizes = jnp.asarray(split_up(count, total, most, skew), jnp.int32)
    couples = (count - 1) // 2
    donor, taker = sizes[1:1 + 2 * couples:2], sizes[2:2 + 2 * couples:2]
    margin = jnp.minimum(donor - 1, most - taker)
    shifted = jax.random.randint(jax.random.fold_in(stream_key, 1), (couples,), 0, 1 << 20) % (margin + 1)
    sizes = sizes.at[1:1 + 2 * couples:2].set(donor - shifted).at[2:2 + 2 * couples:2].set(taker + shifted)
    return sizes[jax.random.permutation(jax.random.fold_in(stream_key, 2), count)]


def normal_values(rng, dims, scale, most, cuts=(), held_as=jnp.bfloat16):
    drawn = scale * jax.random.normal(rng, dims, jnp.float32)
    if cuts:
        drawn = drawn * block_levels(rng, dims, cuts, -0.22, 0.18)
    return jnp.clip(drawn, -most, most).astype(held_as)


def setup_inputs(seed: int = 0) -> dict:
    splits = jax.random.split(jax.random.key(seed), 8)
    tokens = draw_tokens(jax.random.fold_in(splits[7], 71), 0)
    norm_gain = jnp.clip(1.0 + 0.18 * jax.random.normal(splits[1], (D,), jnp.float32), 0.1, 1.9)
    query_weight = draw_query_weight(jax.random.fold_in(splits[7], 71), 0)
    key_weight = draw_key_weight(jax.random.fold_in(splits[7], 71), 0)
    value_weight = normal_values(splits[4], (D, KV_HEADS * HEAD_DIM), D ** -0.5, 0.09375, ((1, 8),))
    out_weight = normal_values(splits[5], (HEADS * HEAD_DIM, D), (HEAD_DIM // 4) ** -0.5, 1.0, ((1, 8),))
    segments = jnp.searchsorted(jnp.cumsum(ragged_sizes(splits[6], 3, TOKENS, TOKENS // 2, 0)), jnp.arange(TOKENS), side="right").astype(jnp.int32)
    return {"tokens": tokens, "norm_gain": norm_gain, "query_weight": query_weight, "key_weight": key_weight, "value_weight": value_weight, "out_weight": out_weight, "segments": segments}


def rotate(vectors, positions):
    half_dim = vectors.shape[-1] // 2
    freqs = 10000.0 ** (-(jnp.arange(half_dim, dtype=jnp.float32) * 2.0 / vectors.shape[-1]))
    angles = positions[:, None] * freqs[None, :]
    cosine = jnp.cos(angles)[:, None, :]
    sine_part = jnp.sin(angles)[:, None, :]
    first = vectors[..., :half_dim]
    second = vectors[..., half_dim:]
    return jnp.concatenate([first * cosine - second * sine_part, second * cosine + first * sine_part], axis=-1)

def project(normed, weight, positions):
    product = jnp.dot(normed, weight, preferred_element_type=jnp.float32)
    shaped = product.reshape(product.shape[0], -1, HEAD_DIM)
    return rotate(shaped, positions).astype(jnp.bfloat16)

def attend(queries, keys, values, allowed):
    block_rows, query_heads, head_size = queries.shape
    value_heads = keys.shape[1]
    grouped = queries.astype(jnp.float32).reshape(block_rows, value_heads, query_heads // value_heads, head_size)
    scores = jnp.einsum('tkgd,skd->kgts', grouped, keys.astype(jnp.float32)) / math.sqrt(head_size)
    scores = jnp.where(allowed[None, None], scores, jnp.float32(-1e+30))
    peak = lax.optimization_barrier(jnp.max(scores, axis=-1, keepdims=True))
    weights = jnp.exp(scores - peak)
    totals = lax.optimization_barrier(jnp.sum(weights, axis=-1, keepdims=True))
    probabilities = (weights / totals).astype(jnp.bfloat16)
    attended = jnp.einsum('kgts,skd->tkgd', probabilities.astype(jnp.float32), values.astype(jnp.float32))
    return attended.reshape(block_rows, query_heads * head_size).astype(jnp.bfloat16)

def reference(tokens, norm_gain, query_weight, key_weight, value_weight, out_weight, segments):
    widened = tokens.astype(jnp.float32)
    scale = lax.rsqrt(lax.optimization_barrier(jnp.mean(widened * widened, axis=-1, keepdims=True)) + 1e-05)
    normed = (widened * scale * norm_gain[None, :]).astype(jnp.bfloat16)
    positions = jnp.arange(TOKENS, dtype=jnp.int32).astype(jnp.float32)
    queries = project(normed, query_weight, positions)
    keys = project(normed, key_weight, positions)
    values = jnp.dot(normed, value_weight, preferred_element_type=jnp.float32).astype(jnp.bfloat16)
    values = values.reshape(TOKENS, KV_HEADS, HEAD_DIM)
    front = HALO * TOK_DEV
    span = (HALO + 1) * TOK_DEV
    padded_keys = jnp.concatenate([jnp.zeros((front, KV_HEADS, HEAD_DIM), jnp.bfloat16), keys], axis=0)
    padded_values = jnp.concatenate([jnp.zeros((front, KV_HEADS, HEAD_DIM), jnp.bfloat16), values], axis=0)
    padded_segments = jnp.concatenate([jnp.full((front,), -1, jnp.int32), segments.astype(jnp.int32)], axis=0)

    def one_block(block):
        start = (block * TOK_DEV).astype(jnp.int32)
        query_block = lax.dynamic_slice_in_dim(queries, start, TOK_DEV, 0)
        key_block = lax.dynamic_slice_in_dim(padded_keys, start, span, 0)
        value_block = lax.dynamic_slice_in_dim(padded_values, start, span, 0)
        query_segments = lax.dynamic_slice_in_dim(segments.astype(jnp.int32), start, TOK_DEV, 0)
        key_segments = lax.dynamic_slice_in_dim(padded_segments, start, span, 0)
        query_pos = start + jnp.arange(TOK_DEV, dtype=jnp.int32)
        key_pos = start - front + jnp.arange(span, dtype=jnp.int32)
        distance = query_pos[:, None] - key_pos[None, :]
        allowed = (distance >= 0) & (distance < WINDOW) & (key_segments[None, :] == query_segments[:, None])
        return attend(query_block, key_block, value_block, allowed)
    attended = lax.map(one_block, jnp.arange(N_SEQ, dtype=jnp.int32)).reshape(TOKENS, HEADS * HEAD_DIM)
    return jnp.dot(attended, out_weight, preferred_element_type=jnp.float32).astype(jnp.bfloat16)
```

```python
import functools
import math

import jax
import jax.numpy as jnp
from jax import lax
from jax.experimental import pallas as pl
from jax.experimental.pallas import tpu as pltpu
from jax.sharding import PartitionSpec as P

HEAD_DIM = 128
WINDOW = 4096
EPSILON = 1e-05


def rotation(positions):
    half_dim = HEAD_DIM // 2
    freqs = 10000.0 ** (-(jnp.arange(half_dim, dtype=jnp.float32) * 2.0 / HEAD_DIM))
    angles = positions[:, None] * freqs[None, :]
    return jnp.cos(angles)[:, None, :], jnp.sin(angles)[:, None, :]


def rotate(product, cosine, sine):
    half_dim = HEAD_DIM // 2
    vectors = product.reshape(product.shape[0], -1, HEAD_DIM)
    first, second = vectors[..., :half_dim], vectors[..., half_dim:]
    turned = jnp.concatenate(
        [first * cosine - second * sine, second * cosine + first * sine], axis=-1
    )
    return turned.reshape(product.shape).astype(jnp.bfloat16)


def attend_kernel(query_heads, kv_heads, back, tile, windowed, q_ref, sq_ref, sk_ref, *refs):
    kv_refs, out_ref = refs[:-1], refs[-1]
    rows, half = q_ref.shape[0], kv_refs[0].shape[0]
    factor = math.log2(math.e) / math.sqrt(HEAD_DIM)
    group = query_heads // kv_heads
    for row in range(0, rows, tile):
        sq = sq_ref[row : row + tile, :]
        masks = []
        for place in range(back + 1):
            mask = sk_ref[:, place * half : (place + 1) * half] == sq
            gap = (back - place) * half + row
            if place == back or windowed:
                distance = (
                    gap
                    + lax.broadcasted_iota(jnp.int32, (tile, half), 0)
                    - lax.broadcasted_iota(jnp.int32, (tile, half), 1)
                )
                if place == back:
                    mask = mask & (distance >= 0)
                if windowed and gap + tile - 1 >= WINDOW:
                    mask = mask & (distance < WINDOW)
            masks.append(mask)
        for head in range(query_heads):
            kv_head = head // group
            q = q_ref[row : row + tile, head * HEAD_DIM : (head + 1) * HEAD_DIM]
            keys = slice(kv_head * HEAD_DIM, (kv_head + 1) * HEAD_DIM)
            vals = slice((kv_heads + kv_head) * HEAD_DIM, (kv_heads + kv_head + 1) * HEAD_DIM)
            scores = []
            for mask, kv in zip(masks, kv_refs):
                s = lax.dot_general(
                    q, kv[:, keys], (((1,), (1,)), ((), ())), preferred_element_type=jnp.float32
                )
                scores.append(jnp.where(mask, s * factor, jnp.float32(-1e30)))
            peak = functools.reduce(jnp.maximum, [jnp.max(s, axis=-1, keepdims=True) for s in scores])
            total, summed = 0.0, 0.0
            for s, kv in zip(scores, kv_refs):
                w = jnp.exp2(s - peak)
                total = total + jnp.sum(w, axis=-1, keepdims=True)
                summed = summed + jnp.dot(
                    w.astype(jnp.bfloat16), kv[:, vals], preferred_element_type=jnp.float32
                )
            out_ref[row : row + tile, head * HEAD_DIM : (head + 1) * HEAD_DIM] = (
                summed / total
            ).astype(jnp.bfloat16)


def attend(queries, part, seg_q, seg_k, key_values, windowed):
    half, width = queries.shape[0] // 2, queries.shape[1]
    back = len(key_values) - 1
    kv_heads = key_values[0].shape[1] // (2 * HEAD_DIM)
    whole = lambda a: pl.BlockSpec(a.shape, lambda i: (0,) * a.ndim)
    return pl.pallas_call(
        functools.partial(attend_kernel, width // HEAD_DIM, kv_heads, back, min(half, 128), windowed),
        grid=(1,),
        out_shape=jax.ShapeDtypeStruct((half, width), jnp.bfloat16),
        in_specs=[pl.BlockSpec((half, width), lambda i: (part, 0)), whole(seg_q), whole(seg_k)]
        + [whole(kv) for kv in key_values],
        out_specs=pl.BlockSpec((half, width), lambda i: (0, 0)),
        name=f"attend{part}",
    )(queries, seg_q, seg_k, *key_values)


def shards(tokens, norm_gain, query_weight, key_weight, value_weight, out_weight, segments):
    block_rows = tokens.shape[0]
    half = block_rows // 2
    seq_index, seq_count = lax.axis_index("seq"), lax.axis_size("seq")
    tp_index, tp_count = lax.axis_index("tp"), lax.axis_size("tp")
    total = block_rows * seq_count
    reach = min(WINDOW, total // 2)
    back = min((reach - 2) // half + 1, 2 * seq_count - 1)
    windowed = total // 2 > WINDOW
    ring = [(i, (i + 1) % seq_count) for i in range(seq_count)]

    widened = tokens.astype(jnp.float32)
    scale = lax.rsqrt(jnp.mean(widened * widened, axis=-1, keepdims=True) + EPSILON)
    normed = (widened * scale * norm_gain[None, :]).astype(jnp.bfloat16)
    positions = (seq_index * block_rows + jnp.arange(block_rows, dtype=jnp.int32)).astype(jnp.float32)
    cosine, sine = rotation(positions)
    keys = rotate(jnp.dot(normed, key_weight, preferred_element_type=jnp.float32), cosine, sine)
    values = jnp.dot(normed, value_weight, preferred_element_type=jnp.float32).astype(jnp.bfloat16)
    own = [
        jnp.concatenate([keys[h * half : (h + 1) * half], values[h * half : (h + 1) * half]], axis=1)
        for h in range(2)
    ]
    halves = [own[1], own[0]]
    for distance in range(2, back + 2):
        halves.append(lax.ppermute(halves[distance - 2], "seq", ring))
    queries = rotate(jnp.dot(normed, query_weight, preferred_element_type=jnp.float32), cosine, sine)
    padded = jnp.concatenate([jnp.full((back * half,), -1, jnp.int32), segments])

    def swap(x, bit):
        return lax.ppermute(x, "tp", [(i, i ^ bit) for i in range(tp_count)])

    width = queries.shape[1]

    def product(x, bits):
        rows = lax.dynamic_slice_in_dim(out_weight, (tp_index ^ bits) * width, width, 0)
        return jnp.dot(x, rows, preferred_element_type=jnp.float32)

    outs = {}
    for part in (1, 0):
        first = (2 * seq_index + part) * half
        seg_k = lax.dynamic_slice_in_dim(padded, first, (back + 1) * half)[None, :]
        seg_q = lax.dynamic_slice_in_dim(segments, first, half)[:, None]
        parts = halves[1 - part : 1 - part + back + 1][::-1]
        mine = attend(queries, part, seg_q, seg_k, parts, windowed)
        got = {0: mine, 2: swap(mine, 2), 4: swap(mine, 4)}
        got[6] = swap(got[4], 2) if part == 1 else swap(got[2], 4)
        acc = None
        for bits in (0, 2, 4, 6):
            both = product(got[bits], bits) + product(swap(got[bits], 1), bits ^ 1)
            acc = both if acc is None else acc + both
        outs[part] = acc.astype(jnp.bfloat16)
    return jnp.concatenate([outs[0], outs[1]], axis=0)


def solution(mesh):
    return jax.shard_map(
        shards,
        mesh=mesh,
        in_specs=(P("seq", None), P(), P(None, "tp"), P(None, "tp"), P(None, "tp"), P(None, "tp"), P()),
        out_specs=P("seq", "tp"),
        check_vma=False,
    )
```

```python
import functools
import math

import jax
import jax.numpy as jnp
import numpy as np
from jax import lax
from jax.experimental import pallas as pl
from jax.experimental.pallas import tpu as pltpu
from jax.sharding import PartitionSpec as P

HEAD_DIM = 128
WINDOW = 4096
EPSILON = 1e-05
BASE = 10000.0


VMEM = pl.BlockSpec(memory_space=pltpu.VMEM)
ANY = pl.BlockSpec(memory_space=pl.ANY)


def rotation_tables(block_rows, blocks):
    freqs = BASE ** (-2.0 * (np.arange(HEAD_DIM) % (HEAD_DIM // 2)) / HEAD_DIM)
    row = np.arange(block_rows)[:, None] * freqs
    start = (np.arange(blocks) * block_rows)[:, None] * freqs
    tables = (np.cos(row), np.sin(row), np.cos(start), np.sin(start))
    return [jnp.asarray(t, jnp.float32) for t in tables]


def rotation(rows, row_cos, row_sin, start_cos, start_sin):
    block = lax.axis_index("seq")
    cos_b, sin_b = start_cos[pl.ds(block, 1), :], start_sin[pl.ds(block, 1), :]
    cos_r, sin_r = row_cos[rows, :], row_sin[rows, :]
    lane = lax.broadcasted_iota(jnp.int32, cos_r.shape, 1)
    sine = sin_r * cos_b + cos_r * sin_b
    return cos_r * cos_b - sin_r * sin_b, jnp.where(lane < HEAD_DIM // 2, -sine, sine)


def rotate(x, cosine, sine):
    return (x * cosine + pltpu.roll(x, HEAD_DIM // 2, 1) * sine).astype(jnp.bfloat16)


def heads_of(width):
    return [slice(h, h + HEAD_DIM) for h in range(0, width, HEAD_DIM)]


def key_value_kernel(part, tile, tokens, gain, key_weight, value_weight, rc, rs, sc, ss, kv_ref, normed_ref, held, sems):
    rows = kv_ref.shape[0]
    width = key_weight.shape[1]
    steps = rows // tile

    def copy(i):
        return pltpu.make_async_copy(
            tokens.at[pl.ds(part * rows + i * tile, tile), :], held.at[pl.ds(i * tile, tile), :], sems.at[i]
        )

    for i in range(steps):
        copy(i).start()
    for i in range(steps):
        copy(i).wait()
        here = slice(i * tile, (i + 1) * tile)
        wide = held[here, :].astype(jnp.float32)
        scale = lax.rsqrt(jnp.mean(wide * wide, axis=-1, keepdims=True) + EPSILON)
        normed = (wide * scale * gain[...]).astype(jnp.bfloat16)
        normed_ref[here, :] = normed
        keys = jnp.dot(normed, key_weight[...], preferred_element_type=jnp.float32)
        values = jnp.dot(normed, value_weight[...], preferred_element_type=jnp.float32)
        cosine, sine = rotation(slice(part * rows + i * tile, part * rows + (i + 1) * tile), rc, rs, sc, ss)
        for h in heads_of(width):
            kv_ref[here, h] = rotate(keys[:, h], cosine, sine)
        kv_ref[here, width:] = values.astype(jnp.bfloat16)


def key_value(part, tokens, gain, key_weight, value_weight, tables):
    half, depth = tokens.shape[0] // 2, tokens.shape[1]
    tile = min(half, 64)
    return pl.pallas_call(
        functools.partial(key_value_kernel, part, tile),
        out_shape=(
            jax.ShapeDtypeStruct((half, 2 * key_weight.shape[1]), jnp.bfloat16),
            jax.ShapeDtypeStruct((half, depth), jnp.bfloat16),
        ),
        in_specs=[ANY] + [VMEM] * 7,
        out_specs=(VMEM, VMEM),
        scratch_shapes=[pltpu.VMEM((half, depth), jnp.bfloat16), pltpu.SemaphoreType.DMA((half // tile,))],
        name=f"key_value{part}",
    )(tokens, gain, key_weight, value_weight, *tables)


def query_kernel(part, normed, weight, rc, rs, sc, ss, out_ref):
    rows = normed.shape[0]
    cosine, sine = rotation(slice(part * rows, (part + 1) * rows), rc, rs, sc, ss)
    product = jnp.dot(normed[...], weight[...], preferred_element_type=jnp.float32)
    for h in heads_of(weight.shape[1]):
        out_ref[:, h] = rotate(product[:, h], cosine, sine)


def query(part, normed, weight, tables):
    return pl.pallas_call(
        functools.partial(query_kernel, part),
        out_shape=jax.ShapeDtypeStruct((normed.shape[0], weight.shape[1]), jnp.bfloat16),
        in_specs=[VMEM] * 6,
        out_specs=VMEM,
        name=f"query{part}",
    )(normed, weight, *tables)


def attend_kernel(back, windowed, q_ref, sq_ref, sk_ref, *refs):
    kv_refs, out_ref, bias_ref = refs[:-2], refs[-2], refs[-1]
    rows, half = q_ref.shape[0], kv_refs[0].shape[0]
    kv_width = kv_refs[0].shape[1] // 2
    group = q_ref.shape[1] // kv_width
    factor = math.log2(math.e) / math.sqrt(HEAD_DIM)
    places = [slice(p * half, (p + 1) * half) for p in range(back + 1)]
    sq = sq_ref[...]
    for place, span in enumerate(places):
        mask = sk_ref[:, span] == sq
        gap = (back - place) * half
        if place == back or (windowed and gap + rows > WINDOW):
            distance = (
                gap
                + lax.broadcasted_iota(jnp.int32, (rows, half), 0)
                - lax.broadcasted_iota(jnp.int32, (rows, half), 1)
            )
            mask = mask & (distance >= 0) & (distance < WINDOW)
        bias_ref[:, span] = jnp.where(mask, jnp.float32(0), jnp.float32(-1e30))
    ones = jnp.ones((half, HEAD_DIM), jnp.bfloat16)
    for h, head in enumerate(heads_of(q_ref.shape[1])):
        first = (h // group) * HEAD_DIM
        keys, vals = slice(first, first + HEAD_DIM), slice(kv_width + first, kv_width + first + HEAD_DIM)
        q = q_ref[:, head]
        scores = [
            lax.dot_general(q, kv[:, keys], (((1,), (1,)), ((), ())), preferred_element_type=jnp.float32)
            * factor
            + bias_ref[:, span]
            for kv, span in zip(kv_refs, places)
        ]
        peak = jnp.max(functools.reduce(jnp.maximum, scores), axis=-1, keepdims=True)
        summed = 0.0
        for s, kv in zip(scores, kv_refs):
            w = jnp.exp2(s - peak).astype(jnp.bfloat16)
            both = jnp.concatenate([kv[:, vals], ones], axis=1)
            summed = summed + jnp.dot(w, both, preferred_element_type=jnp.float32)
        out_ref[:, head] = (summed[:, :HEAD_DIM] / summed[:, HEAD_DIM:]).astype(jnp.bfloat16)


def attend(part, queries, seg_q, seg_k, key_values, windowed):
    half = queries.shape[0]
    back = len(key_values) - 1
    return pl.pallas_call(
        functools.partial(attend_kernel, back, windowed),
        out_shape=jax.ShapeDtypeStruct(queries.shape, jnp.bfloat16),
        in_specs=[VMEM] * (3 + len(key_values)),
        out_specs=VMEM,
        scratch_shapes=[pltpu.VMEM((half, (back + 1) * half), jnp.float32)],
        name=f"attend{part}",
    )(queries, seg_q, seg_k, *key_values)


def product_kernel(bits, last, weight, *refs):
    xs, out_ref = refs[: len(bits)], refs[-1]
    depth = xs[0].shape[1]
    me = lax.axis_index("tp")
    total = refs[len(bits)][...] if len(refs) > len(bits) + 1 else 0.0
    for bit, x in zip(bits, xs):
        owner = jnp.bitwise_xor(me, bit)
        rows = pl.ds(pl.multiple_of(owner * depth, depth), depth)
        total = total + jnp.dot(x[...], weight[rows, :], preferred_element_type=jnp.float32)
    out_ref[...] = total.astype(out_ref.dtype)


def product(weight, got, total, last, name):
    bits, xs = zip(*got)
    extra = () if total is None else (total,)
    return pl.pallas_call(
        functools.partial(product_kernel, bits, last),
        out_shape=jax.ShapeDtypeStruct((xs[0].shape[0], weight.shape[1]), jnp.bfloat16 if last else jnp.float32),
        in_specs=[VMEM] * (1 + len(xs) + len(extra)),
        out_specs=VMEM,
        name=name,
    )(weight, *xs, *extra)


def shards(tokens, norm_gain, query_weight, key_weight, value_weight, out_weight, segments):
    block_rows = tokens.shape[0]
    half = block_rows // 2
    seq_index, seq_count = lax.axis_index("seq"), lax.axis_size("seq")
    tp_count = lax.axis_size("tp")
    total = block_rows * seq_count
    reach = min(WINDOW, total // 2)
    back = min((reach - 2) // half + 1, 2 * seq_count - 1)
    windowed = total // 2 > WINDOW
    ring = [(i, (i + 1) % seq_count) for i in range(seq_count)]
    tables = rotation_tables(block_rows, seq_count)
    gain = norm_gain[None, :]

    halves, normed = [None] * (back + 2), [None, None]
    for part in (1, 0):
        halves[1 - part], normed[part] = key_value(part, tokens, gain, key_weight, value_weight, tables)
    for distance in range(2, back + 2):
        halves[distance] = lax.ppermute(halves[distance - 2], "seq", ring)
    padded = jnp.concatenate([jnp.full((back * half,), -1, jnp.int32), segments])

    def swap(x, bit):
        return lax.ppermute(x, "tp", [(i, i ^ bit) for i in range(tp_count)])

    outs = {}
    for part in (1, 0):
        queries = query(part, normed[part], query_weight, tables)
        first = (2 * seq_index + part) * half
        seg_k = lax.dynamic_slice_in_dim(padded, first, (back + 1) * half)[None, :]
        seg_q = lax.dynamic_slice_in_dim(segments, first, half)[:, None]
        parts = halves[1 - part : 1 - part + back + 1][::-1]
        mine = attend(part, queries, seg_q, seg_k, parts, windowed)
        got = {0: mine, 2: swap(mine, 2), 4: swap(mine, 4)}
        got[6] = swap(got[4], 2) if part == 1 else swap(got[2], 4)
        for bits in (0, 2, 4, 6):
            got[bits | 1] = swap(got[bits], 1)
        acc = product(out_weight, [(b, got[b]) for b in (0, 1)], None, False, f"product{part}a")
        acc = product(out_weight, [(b, got[b]) for b in (2, 3, 4, 5)], acc, False, f"product{part}b")
        outs[part] = product(out_weight, [(b, got[b]) for b in (6, 7)], acc, True, f"product{part}c")
    return jnp.concatenate([outs[0], outs[1]], axis=0)


def solution(mesh):
    return jax.shard_map(
        shards,
        mesh=mesh,
        in_specs=(P("seq", None), P(), P(None, "tp"), P(None, "tp"), P(None, "tp"), P(None, "tp"), P()),
        out_specs=P("seq", "tp"),
        check_vma=False,
    )
```

```python
import functools
import math

import jax
import jax.numpy as jnp
import numpy as np
from jax import lax
from jax.experimental import pallas as pl
from jax.experimental.pallas import tpu as pltpu
from jax.sharding import PartitionSpec as P

HEAD_DIM = 128
WINDOW = 4096
EPSILON = 1e-05
BASE = 10000.0


VMEM = pl.BlockSpec(memory_space=pltpu.VMEM)
HBM = pl.BlockSpec(memory_space=pltpu.HBM)
PARAMS = pltpu.CompilerParams(vmem_limit_bytes=16 << 20)


def in_hbm(*arrays):
    return [pltpu.with_memory_space_constraint(a, pltpu.HBM) for a in arrays]


def rotation_tables(block_rows, blocks):
    freqs = BASE ** (-2.0 * (np.arange(HEAD_DIM) % (HEAD_DIM // 2)) / HEAD_DIM)
    row = np.arange(block_rows)[:, None] * freqs
    start = (np.arange(blocks) * block_rows)[:, None] * freqs
    tables = (np.cos(row), np.sin(row), np.cos(start), np.sin(start))
    return [jnp.asarray(t, jnp.float32) for t in tables]


def rotate(x, cosine, sine):
    return (x * cosine + pltpu.roll(x, HEAD_DIM // 2, 1) * sine).astype(jnp.bfloat16)


def heads_of(width):
    return [slice(h, h + HEAD_DIM) for h in range(0, width, HEAD_DIM)]


def normalise(tokens, gain):
    wide = tokens.astype(jnp.float32)
    scale = lax.rsqrt(jnp.mean(wide * wide, axis=-1, keepdims=True) + EPSILON)
    return (wide * scale * gain).astype(jnp.bfloat16)


def key_value_of(normed, weight, cosine, sine, kv_ref, here):
    product = jnp.dot(normed, weight, preferred_element_type=jnp.float32)
    width = kv_ref.shape[1] // 2
    for h in heads_of(width):
        kv_ref[here, h] = rotate(product[:, h], cosine, sine)
    kv_ref[here, width:] = product[:, width:].astype(jnp.bfloat16)


def second_half_kernel(
    tile, tokens, gain, key_weight, value_weight, row_cos, row_sin, start_cos, start_sin,
    kv_ref, normed_ref, weight, first_tokens, gain_copy, cosine, sine,
    held, row_c, row_s, start_c, start_s, tile_sems, sems,
):
    rows, width = kv_ref.shape[0], key_weight.shape[1]
    steps = rows // tile
    tiles = [
        pltpu.make_async_copy(
            tokens.at[rows + i * tile : rows + (i + 1) * tile, :],
            held.at[i * tile : (i + 1) * tile, :],
            tile_sems.at[i],
        )
        for i in range(steps)
    ]
    moves = [
        (gain, gain_copy),
        (key_weight, weight.at[:, :width]),
        (value_weight, weight.at[:, width:]),
        (row_cos, row_c),
        (row_sin, row_s),
        (start_cos, start_c),
        (start_sin, start_s),
        (tokens.at[:rows, :], first_tokens),
    ]
    moves = [pltpu.make_async_copy(a, b, sems.at[i]) for i, (a, b) in enumerate(moves)]
    tiles[0].start()
    moves[0].start()
    for move in moves[1:3]:
        move.start()
    for copy in tiles[1:]:
        copy.start()
    for move in moves[3:]:
        move.start()
    moves[0].wait()
    for i in range(steps):
        here = slice(i * tile, (i + 1) * tile)
        tiles[i].wait()
        normed_ref[here, :] = normalise(held[here, :], gain_copy[...])
    for move in moves[3:7]:
        move.wait()
    block = lax.axis_index("seq")
    cos_b, sin_b = start_c[pl.ds(block, 1), :], start_s[pl.ds(block, 1), :]
    cos_r, sin_r = row_c[...], row_s[...]
    lane = lax.broadcasted_iota(jnp.int32, cos_r.shape, 1)
    cosine[...] = cos_r * cos_b - sin_r * sin_b
    turned = sin_r * cos_b + cos_r * sin_b
    sine[...] = jnp.where(lane < HEAD_DIM // 2, -turned, turned)
    moves[1].wait()
    moves[2].wait()
    key_value_of(normed_ref[...], weight[...], cosine[rows:, :], sine[rows:, :], kv_ref, slice(None))
    moves[7].wait()


def second_half(tokens, gain, key_weight, value_weight, tables):
    block_rows, depth = tokens.shape
    half, width = block_rows // 2, key_weight.shape[1]
    tile = min(half, 64)
    shape, bf16, f32 = jax.ShapeDtypeStruct, jnp.bfloat16, jnp.float32
    return pl.pallas_call(
        functools.partial(second_half_kernel, tile),
        out_shape=(
            shape((half, 2 * width), bf16),
            shape((half, depth), bf16),
            shape((depth, 2 * width), bf16),
            shape((half, depth), bf16),
            shape(gain.shape, f32),
            shape((block_rows, HEAD_DIM), f32),
            shape((block_rows, HEAD_DIM), f32),
        ),
        in_specs=[HBM] * 8,
        out_specs=(VMEM,) * 7,
        scratch_shapes=[pltpu.VMEM((half, depth), bf16)]
        + [pltpu.VMEM(t.shape, f32) for t in tables]
        + [pltpu.SemaphoreType.DMA((half // tile,)), pltpu.SemaphoreType.DMA((8,))],
        compiler_params=PARAMS,
        name="second_half",
    )(*in_hbm(tokens, gain, key_weight, value_weight, *tables))


def first_half_kernel(tokens, gain, weight, cosine, sine, query_weight, kv_ref, normed_ref, query_copy, sem):
    move = pltpu.make_async_copy(query_weight, query_copy, sem)
    move.start()
    rows = kv_ref.shape[0]
    normed_ref[...] = normalise(tokens[...], gain[...])
    key_value_of(normed_ref[...], weight[...], cosine[:rows, :], sine[:rows, :], kv_ref, slice(None))
    move.wait()


def first_half(tokens, gain, weight, cosine, sine, query_weight):
    half = tokens.shape[0]
    return pl.pallas_call(
        first_half_kernel,
        out_shape=(
            jax.ShapeDtypeStruct((half, weight.shape[1]), jnp.bfloat16),
            jax.ShapeDtypeStruct(tokens.shape, jnp.bfloat16),
            jax.ShapeDtypeStruct(query_weight.shape, jnp.bfloat16),
        ),
        in_specs=[VMEM] * 5 + [HBM],
        out_specs=(VMEM,) * 3,
        scratch_shapes=[pltpu.SemaphoreType.DMA],
        compiler_params=PARAMS,
        name="first_half",
    )(tokens, gain, weight, cosine, sine, *in_hbm(query_weight))


def query_kernel(part, normed, weight, cosine, sine, out_ref):
    rows = slice(part * normed.shape[0], (part + 1) * normed.shape[0])
    product = jnp.dot(normed[...], weight[...], preferred_element_type=jnp.float32)
    for h in heads_of(weight.shape[1]):
        out_ref[:, h] = rotate(product[:, h], cosine[rows, :], sine[rows, :])


def query(part, normed, weight, cosine, sine):
    return pl.pallas_call(
        functools.partial(query_kernel, part),
        out_shape=jax.ShapeDtypeStruct((normed.shape[0], weight.shape[1]), jnp.bfloat16),
        in_specs=[VMEM] * 4,
        out_specs=VMEM,
        compiler_params=PARAMS,
    )(normed, weight, cosine, sine)


def attend_kernel(part, back, limits, q_ref, *refs):
    kv_refs, out_ref, bias_ref = refs[:-2], refs[-2], refs[-1]
    rows, half = q_ref.shape[0], kv_refs[0].shape[0]
    kv_width = kv_refs[0].shape[1] // 2
    group = q_ref.shape[1] // kv_width
    factor = math.log2(math.e) / math.sqrt(HEAD_DIM)
    places = [slice(p * half, (p + 1) * half) for p in range(back + 1)]
    base = (2 * lax.axis_index("seq") + part) * half
    row = base + lax.broadcasted_iota(jnp.int32, (rows, HEAD_DIM), 0)
    start = jnp.where(row >= limits[1], limits[1], jnp.where(row >= limits[0], limits[0], 0))
    start = jnp.maximum(start, row - (WINDOW - 1))
    for place, span in enumerate(places):
        first = base - (back - place) * half
        for left in range(0, half, HEAD_DIM):
            key = first + left + lax.broadcasted_iota(jnp.int32, (rows, HEAD_DIM), 1)
            mask = key >= start
            if place == back:
                mask = mask & (key <= row)
            bias_ref[:, place * half + left : place * half + left + HEAD_DIM] = jnp.where(
                mask, jnp.float32(0), jnp.float32(-1e30)
            )
    ones = jnp.ones((half, HEAD_DIM), jnp.bfloat16)
    for h, head in enumerate(heads_of(q_ref.shape[1])):
        first = (h // group) * HEAD_DIM
        keys, vals = slice(first, first + HEAD_DIM), slice(kv_width + first, kv_width + first + HEAD_DIM)
        q = q_ref[:, head]
        scores = [
            lax.dot_general(q, kv[:, keys], (((1,), (1,)), ((), ())), preferred_element_type=jnp.float32)
            * factor
            + bias_ref[:, span]
            for kv, span in zip(kv_refs, places)
        ]
        peak = jnp.max(functools.reduce(jnp.maximum, scores), axis=-1, keepdims=True)
        summed = 0.0
        for s, kv in zip(scores, kv_refs):
            w = jnp.exp2(s - peak).astype(jnp.bfloat16)
            both = jnp.concatenate([kv[:, vals], ones], axis=1)
            summed = summed + jnp.dot(w, both, preferred_element_type=jnp.float32)
        out_ref[:, head] = (summed[:, :HEAD_DIM] / summed[:, HEAD_DIM:]).astype(jnp.bfloat16)


def attend(part, queries, limits, key_values):
    half = queries.shape[0]
    back = len(key_values) - 1
    return pl.pallas_call(
        functools.partial(attend_kernel, part, back),
        out_shape=jax.ShapeDtypeStruct(queries.shape, jnp.bfloat16),
        in_specs=[pl.BlockSpec(memory_space=pltpu.SMEM)] + [VMEM] * (1 + len(key_values)),
        out_specs=VMEM,
        scratch_shapes=[pltpu.VMEM((half, (back + 1) * half), jnp.float32)],
        compiler_params=PARAMS,
    )(limits, queries, *key_values)


def added(bits, total, weight, xs):
    depth = xs[0].shape[1]
    me = lax.axis_index("tp")
    for bit, x in zip(bits, xs):
        owner = jnp.bitwise_xor(me, bit)
        rows = pl.ds(pl.multiple_of(owner * depth, depth), depth)
        total = total + jnp.dot(x[...], weight[rows, :], preferred_element_type=jnp.float32)
    return total


def product_kernel(bits, extra, weight, *refs):
    xs, out_ref = refs[: len(bits)], refs[-1]
    out_ref[...] = added(bits, refs[len(bits)][...] if extra else 0.0, weight, xs)


def product(weight, got, total=None):
    bits, xs = zip(*got)
    extra = () if total is None else (total,)
    return pl.pallas_call(
        functools.partial(product_kernel, bits, bool(extra)),
        out_shape=jax.ShapeDtypeStruct((xs[0].shape[0], weight.shape[1]), jnp.float32),
        in_specs=[VMEM] * (1 + len(xs) + len(extra)),
        out_specs=VMEM,
        compiler_params=PARAMS,
    )(weight, *xs, *extra)


def store_kernel(part, bits, weight, *refs):
    xs, total = refs[: len(bits)], refs[len(bits)]
    out_ref, rounded, sem = refs[-3:]
    rounded[...] = added(bits, total[...], weight, xs).astype(rounded.dtype)
    half = rounded.shape[0]
    move = pltpu.make_async_copy(rounded, out_ref.at[part * half : (part + 1) * half, :], sem)
    move.start()
    move.wait()


def store(part, weight, got, total, out=None):
    bits, xs = zip(*got)
    half, width = total.shape
    extra = () if out is None else in_hbm(out)
    count = 2 + len(xs)
    return pl.pallas_call(
        functools.partial(store_kernel, part, bits),
        out_shape=pltpu.HBM((2 * half, width), jnp.bfloat16),
        in_specs=[VMEM] * count + [HBM] * len(extra),
        out_specs=HBM,
        scratch_shapes=[pltpu.VMEM((half, width), jnp.bfloat16), pltpu.SemaphoreType.DMA],
        input_output_aliases={count: 0} if extra else {},
        compiler_params=PARAMS,
    )(weight, *xs, total, *extra)


def shards(tokens, norm_gain, query_weight, key_weight, value_weight, out_weight, segments):
    block_rows = tokens.shape[0]
    half = block_rows // 2
    seq_count, tp_count = lax.axis_size("seq"), lax.axis_size("tp")
    total = block_rows * seq_count
    reach = min(WINDOW, total // 2)
    back = min((reach - 2) // half + 1, 2 * seq_count - 1)
    ring = [(i, (i + 1) % seq_count) for i in range(seq_count)]
    limits = jnp.sum((segments[None, :] < jnp.array([[1], [2]], jnp.int32)).astype(jnp.int32), axis=1)

    halves, normed, queries = [None] * (back + 2), [None, None], [None, None]
    halves[0], normed[1], weight, first_tokens, gain, cosine, sine = second_half(
        tokens, norm_gain[None, :], key_weight, value_weight, rotation_tables(block_rows, seq_count)
    )
    halves[1], normed[0], query_copy = first_half(first_tokens, gain, weight, cosine, sine, query_weight)
    for distance in range(2, back + 2):
        halves[distance] = lax.ppermute(halves[distance - 2], "seq", ring)
    for part in (1, 0):
        queries[part] = query(part, normed[part], query_copy, cosine, sine)

    def swap(x, bit):
        return lax.ppermute(x, "tp", [(i, i ^ bit) for i in range(tp_count)])

    got, out = {}, None
    for part in (1, 0):
        mine = attend(part, queries[part], limits, halves[1 - part : 1 - part + back + 1][::-1])
        has = got[part] = {0: mine, 2: swap(mine, 2), 4: swap(mine, 4)}
        has[6] = swap(has[4], 2) if part == 1 else swap(has[2], 4)
        for bits in (0, 2, 4, 6):
            has[bits | 1] = swap(has[bits], 1)
    for part in (1, 0):
        pieces = lambda *bits: [(b, got[part][b]) for b in bits]
        acc = None
        for bits in ((0, 1), (2, 3, 4, 5), (6,)):
            acc = product(out_weight, pieces(*bits), acc)
        out = store(part, out_weight, pieces(7), acc, out)
    return out


def solution(mesh):
    return jax.shard_map(
        shards,
        mesh=mesh,
        in_specs=(P("seq", None), P(), P(None, "tp"), P(None, "tp"), P(None, "tp"), P(None, "tp"), P()),
        out_specs=P("seq", "tp"),
        check_vma=False,
    )
```

```python
import functools
import math

import jax
import jax.numpy as jnp
import numpy as np
from jax import lax
from jax.experimental import pallas as pl
from jax.experimental.pallas import tpu as pltpu
from jax.sharding import PartitionSpec as P

HEAD_DIM = 128
WINDOW = 4096
EPSILON = 1e-05
BASE = 10000.0


VMEM = pl.BlockSpec(memory_space=pltpu.VMEM)
HBM = pl.BlockSpec(memory_space=pltpu.HBM)
PARAMS = pltpu.CompilerParams(vmem_limit_bytes=16 << 20)


def in_hbm(*arrays):
    return [pltpu.with_memory_space_constraint(a, pltpu.HBM) for a in arrays]


def rotation_tables(block_rows, blocks):
    freqs = BASE ** (-2.0 * (np.arange(HEAD_DIM) % (HEAD_DIM // 2)) / HEAD_DIM)
    row = np.arange(block_rows)[:, None] * freqs
    start = (np.arange(blocks) * block_rows)[:, None] * freqs
    tables = (np.cos(row), np.sin(row), np.cos(start), np.sin(start))
    return [jnp.asarray(t, jnp.float32) for t in tables]


def rotate(x, cosine, sine):
    return (x * cosine + pltpu.roll(x, HEAD_DIM // 2, 1) * sine).astype(jnp.bfloat16)


def heads_of(width):
    return [slice(h, h + HEAD_DIM) for h in range(0, width, HEAD_DIM)]


def normalise(tokens, gain):
    wide = tokens.astype(jnp.float32)
    scale = lax.rsqrt(jnp.mean(wide * wide, axis=-1, keepdims=True) + EPSILON)
    return (wide * scale * gain).astype(jnp.bfloat16)


def key_value_of(normed, weight, cosine, sine, kv_ref, here):
    product = jnp.dot(normed, weight, preferred_element_type=jnp.float32)
    width = kv_ref.shape[1] // 2
    for h in heads_of(width):
        kv_ref[here, h] = rotate(product[:, h], cosine, sine)
    kv_ref[here, width:] = product[:, width:].astype(jnp.bfloat16)


def second_half_kernel(
    tile, tokens, gain, key_weight, value_weight, row_cos, row_sin, start_cos, start_sin, segments,
    kv_ref, normed_ref, weight, first_tokens, gain_copy, cosine, sine, limits,
    held, row_c, row_s, start_c, start_s, numbers, tile_sems, sems,
):
    rows, width = kv_ref.shape[0], key_weight.shape[1]
    steps = rows // tile
    tiles = [
        pltpu.make_async_copy(
            tokens.at[rows + i * tile : rows + (i + 1) * tile, :],
            held.at[i * tile : (i + 1) * tile, :],
            tile_sems.at[i],
        )
        for i in range(steps)
    ]
    moves = [
        (gain, gain_copy),
        (key_weight, weight.at[:, :width]),
        (value_weight, weight.at[:, width:]),
        (row_cos, row_c),
        (row_sin, row_s),
        (start_cos, start_c),
        (start_sin, start_s),
        (tokens.at[:rows, :], first_tokens),
        (segments, numbers),
    ]
    moves = [pltpu.make_async_copy(a, b, sems.at[i]) for i, (a, b) in enumerate(moves)]
    for move in [moves[8], moves[0]] + tiles + moves[1:8]:
        move.start()
    moves[8].wait()
    for value in (1, 2):
        before = jnp.sum((numbers[...] < value).astype(jnp.float32), axis=0, keepdims=True)
        count = jnp.broadcast_to(jnp.sum(before, axis=1, keepdims=True), before.shape)
        limits[value - 1 : value, :] = count.astype(jnp.int32)
    moves[0].wait()
    for i in range(steps):
        here = slice(i * tile, (i + 1) * tile)
        tiles[i].wait()
        normed_ref[here, :] = normalise(held[here, :], gain_copy[...])
    for move in moves[3:7]:
        move.wait()
    block = lax.axis_index("seq")
    cos_b, sin_b = start_c[pl.ds(block, 1), :], start_s[pl.ds(block, 1), :]
    cos_r, sin_r = row_c[...], row_s[...]
    lane = lax.broadcasted_iota(jnp.int32, cos_r.shape, 1)
    cosine[...] = cos_r * cos_b - sin_r * sin_b
    turned = sin_r * cos_b + cos_r * sin_b
    sine[...] = jnp.where(lane < HEAD_DIM // 2, -turned, turned)
    moves[1].wait()
    moves[2].wait()
    key_value_of(normed_ref[...], weight[...], cosine[rows:, :], sine[rows:, :], kv_ref, slice(None))
    moves[7].wait()


def second_half(tokens, gain, key_weight, value_weight, tables, segments):
    block_rows, depth = tokens.shape
    half, width = block_rows // 2, key_weight.shape[1]
    tile = min(half, 64)
    shape, bf16, f32 = jax.ShapeDtypeStruct, jnp.bfloat16, jnp.float32
    return pl.pallas_call(
        functools.partial(second_half_kernel, tile),
        out_shape=(
            shape((half, 2 * width), bf16),
            shape((half, depth), bf16),
            shape((depth, 2 * width), bf16),
            shape((half, depth), bf16),
            shape(gain.shape, f32),
            shape((block_rows, HEAD_DIM), f32),
            shape((block_rows, HEAD_DIM), f32),
            shape((2, HEAD_DIM), jnp.int32),
        ),
        in_specs=[HBM] * 9,
        out_specs=(VMEM,) * 8,
        scratch_shapes=[pltpu.VMEM((half, depth), bf16)]
        + [pltpu.VMEM(t.shape, f32) for t in tables]
        + [pltpu.VMEM(segments.shape, jnp.int32)]
        + [pltpu.SemaphoreType.DMA((half // tile,)), pltpu.SemaphoreType.DMA((9,))],
        compiler_params=PARAMS,
        name="second_half",
    )(*in_hbm(tokens, gain, key_weight, value_weight, *tables, segments))


def first_half_kernel(tokens, gain, weight, cosine, sine, kv_ref, normed_ref):
    rows = kv_ref.shape[0]
    normed_ref[...] = normalise(tokens[...], gain[...])
    key_value_of(normed_ref[...], weight[...], cosine[:rows, :], sine[:rows, :], kv_ref, slice(None))


def first_half(tokens, gain, weight, cosine, sine):
    half = tokens.shape[0]
    return pl.pallas_call(
        first_half_kernel,
        out_shape=(
            jax.ShapeDtypeStruct((half, weight.shape[1]), jnp.bfloat16),
            jax.ShapeDtypeStruct(tokens.shape, jnp.bfloat16),
        ),
        in_specs=[VMEM] * 5,
        out_specs=(VMEM,) * 2,
        compiler_params=PARAMS,
        name="first_half",
    )(tokens, gain, weight, cosine, sine)


def query_kernel(part, normed, weight, cosine, sine, out_ref):
    rows = slice(part * normed.shape[0], (part + 1) * normed.shape[0])
    product = jnp.dot(normed[...], weight[...], preferred_element_type=jnp.float32)
    for h in heads_of(weight.shape[1]):
        out_ref[:, h] = rotate(product[:, h], cosine[rows, :], sine[rows, :])


def query(part, normed, weight, cosine, sine):
    return pl.pallas_call(
        functools.partial(query_kernel, part),
        out_shape=jax.ShapeDtypeStruct((normed.shape[0], weight.shape[1]), jnp.bfloat16),
        in_specs=[VMEM] * 4,
        out_specs=VMEM,
        compiler_params=PARAMS,
    )(normed, weight, cosine, sine)


TILE, AHEAD = 256, 3
FACTOR = math.log2(math.e) / math.sqrt(HEAD_DIM)


def bias_of(part, place, back, half, limits, bias_ref, column):
    base = (2 * lax.axis_index("seq") + part) * half
    row = base + lax.broadcasted_iota(jnp.int32, (half, HEAD_DIM), 0)
    starts = [jnp.broadcast_to(limits[i : i + 1, :], row.shape) for i in range(2)]
    start = jnp.where(row >= starts[1], starts[1], jnp.where(row >= starts[0], starts[0], 0))
    start = jnp.maximum(start, row - (WINDOW - 1))
    first = base - (back - place) * half
    for left in range(0, half, HEAD_DIM):
        key = first + left + lax.broadcasted_iota(jnp.int32, (half, HEAD_DIM), 1)
        mask = key >= start
        if place == back:
            mask = mask & (key <= row)
        bias_ref[:, column + left : column + left + HEAD_DIM] = jnp.where(
            mask, jnp.float32(0), jnp.float32(-1e30)
        )


def attend_kernel(part, back, places, early, late, limits, q_ref, *refs):
    kv_refs, refs = refs[: len(places)], refs[len(places) :]
    bias_ref = refs[-1]
    half = q_ref.shape[0]
    kv_width = kv_refs[0].shape[1] // 2
    group = q_ref.shape[1] // kv_width
    for i, place in enumerate(places):
        bias_of(part, place, back, half, limits, bias_ref, i * half)
    ones = jnp.ones((half, HEAD_DIM), jnp.bfloat16)
    tile = min(half, TILE)
    wide = half // HEAD_DIM

    def score(h, rows):
        first = (h // group) * HEAD_DIM
        q = q_ref[rows, h * HEAD_DIM : (h + 1) * HEAD_DIM]
        scores = []
        for i, kv in enumerate(kv_refs):
            s = lax.dot_general(
                q, kv[:, first : first + HEAD_DIM], (((1,), (1,)), ((), ())), preferred_element_type=jnp.float32
            )
            scores.append(s * FACTOR + bias_ref[rows, i * half : (i + 1) * half])
        return scores

    def finish(h, rows, scores):
        first = kv_width + (h // group) * HEAD_DIM
        head = slice(h * HEAD_DIM, (h + 1) * HEAD_DIM)
        pair = slice(2 * h * HEAD_DIM, 2 * (h + 1) * HEAD_DIM)
        top = functools.reduce(jnp.maximum, scores)
        top = functools.reduce(jnp.maximum, [top[:, c * HEAD_DIM : (c + 1) * HEAD_DIM] for c in range(wide)])
        peak = jnp.broadcast_to(jnp.max(top, axis=-1, keepdims=True), top.shape)
        summed = 0.0
        if late:
            before = refs[1][rows, head]
            peak = jnp.maximum(peak, before)
            fade = jnp.exp2(before - peak)
            summed = refs[0][rows, pair] * jnp.concatenate([fade, fade], axis=1)
        peaks = jnp.concatenate([peak] * wide, axis=1)
        for s, kv in zip(scores, kv_refs):
            w = jnp.exp2(s - peaks).astype(jnp.bfloat16)
            both = jnp.concatenate([kv[:, first : first + HEAD_DIM], ones], axis=1)
            summed = summed + jnp.dot(w, both, preferred_element_type=jnp.float32)
        if early:
            refs[0][rows, pair] = summed
            refs[1][rows, head] = peak
        else:
            refs[-2][rows, head] = (summed[:, :HEAD_DIM] / summed[:, HEAD_DIM:]).astype(jnp.bfloat16)

    units = [
        (h, slice(row, row + tile)) for h in range(q_ref.shape[1] // HEAD_DIM) for row in range(0, half, tile)
    ]
    waiting = []
    for unit in units:
        waiting.append((*unit, score(*unit)))
        if len(waiting) > AHEAD:
            finish(*waiting.pop(0))
    for unit in waiting:
        finish(*unit)


def attend(part, back, places, queries, limits, key_values, early=False, before=()):
    half, width = queries.shape
    if early:
        shape = (
            jax.ShapeDtypeStruct((half, 2 * width), jnp.float32),
            jax.ShapeDtypeStruct((half, width), jnp.float32),
        )
    else:
        shape = jax.ShapeDtypeStruct((half, width), jnp.bfloat16)
    key_values = [key_values[p] for p in places]
    return pl.pallas_call(
        functools.partial(attend_kernel, part, back, tuple(places), early, bool(before)),
        out_shape=shape,
        in_specs=[VMEM] * (2 + len(places) + len(before)),
        out_specs=(VMEM, VMEM) if early else VMEM,
        scratch_shapes=[pltpu.VMEM((half, len(places) * half), jnp.float32)],
        compiler_params=pltpu.CompilerParams(vmem_limit_bytes=max(16, 2 * len(places)) << 20),
    )(limits, queries, *key_values, *before)


def added(bits, total, weight, xs):
    depth = xs[0].shape[1]
    me = lax.axis_index("tp")
    for bit, x in zip(bits, xs):
        owner = jnp.bitwise_xor(me, bit)
        rows = pl.ds(pl.multiple_of(owner * depth, depth), depth)
        total = total + jnp.dot(x[...], weight[rows, :], preferred_element_type=jnp.float32)
    return total


def product_kernel(bits, extra, weight, *refs):
    xs, out_ref = refs[: len(bits)], refs[-1]
    out_ref[...] = added(bits, refs[len(bits)][...] if extra else 0.0, weight, xs)


def product(weight, got, total=None):
    bits, xs = zip(*got)
    extra = () if total is None else (total,)
    return pl.pallas_call(
        functools.partial(product_kernel, bits, bool(extra)),
        out_shape=jax.ShapeDtypeStruct((xs[0].shape[0], weight.shape[1]), jnp.float32),
        in_specs=[VMEM] * (1 + len(xs) + len(extra)),
        out_specs=VMEM,
        compiler_params=PARAMS,
    )(weight, *xs, *extra)


def store_kernel(part, bits, weight, *refs):
    xs, total = refs[: len(bits)], refs[len(bits)]
    out_ref, rounded, sem = refs[-3:]
    rounded[...] = added(bits, total[...], weight, xs).astype(rounded.dtype)
    half = rounded.shape[0]
    move = pltpu.make_async_copy(rounded, out_ref.at[part * half : (part + 1) * half, :], sem)
    move.start()
    move.wait()


def store(part, weight, got, total, out=None):
    bits, xs = zip(*got)
    half, width = total.shape
    extra = () if out is None else in_hbm(out)
    count = 2 + len(xs)
    return pl.pallas_call(
        functools.partial(store_kernel, part, bits),
        out_shape=pltpu.HBM((2 * half, width), jnp.bfloat16),
        in_specs=[VMEM] * count + [HBM] * len(extra),
        out_specs=HBM,
        scratch_shapes=[pltpu.VMEM((half, width), jnp.bfloat16), pltpu.SemaphoreType.DMA],
        input_output_aliases={count: 0} if extra else {},
        compiler_params=PARAMS,
    )(weight, *xs, total, *extra)


def shards(tokens, norm_gain, query_weight, key_weight, value_weight, out_weight, segments):
    block_rows = tokens.shape[0]
    half = block_rows // 2
    seq_count, tp_count = lax.axis_size("seq"), lax.axis_size("tp")
    total = block_rows * seq_count
    reach = min(WINDOW, total // 2)
    back = min((reach - 2) // half + 1, 2 * seq_count - 1)
    ring = [(i, (i + 1) % seq_count) for i in range(seq_count)]

    halves, normed, queries = [None] * (back + 2), [None, None], [None, None]
    halves[0], normed[1], weight, first_tokens, gain, cosine, sine, limits = second_half(
        tokens,
        norm_gain[None, :],
        key_weight,
        value_weight,
        rotation_tables(block_rows, seq_count),
        segments.reshape(-1, HEAD_DIM),
    )
    halves[1], normed[0] = first_half(first_tokens, gain, weight, cosine, sine)
    for distance in range(2, back + 2):
        halves[distance] = lax.ppermute(halves[distance - 2], "seq", ring)
    for part in (1, 0):
        queries[part] = query(part, normed[part], query_weight, cosine, sine)

    def swap(x, bit):
        return lax.ppermute(x, "tp", [(i, i ^ bit) for i in range(tp_count)])

    got, out = {}, None
    for part in (1, 0):
        key_values = halves[1 - part : 1 - part + back + 1][::-1]
        if part == 1:
            before = attend(part, back, range(1, back + 1), queries[part], limits, key_values, early=True)
            mine = attend(part, back, [0], queries[part], limits, key_values, before=before)
        else:
            mine = attend(part, back, range(back + 1), queries[part], limits, key_values)
        has = got[part] = {0: mine, 2: swap(mine, 2), 4: swap(mine, 4)}
        has[6] = swap(has[4], 2) if part == 0 else swap(has[2], 4)
        for bits in (0, 2, 4, 6):
            has[bits | 1] = swap(has[bits], 1)
    for part in (1, 0):
        pieces = lambda *bits: [(b, got[part][b]) for b in bits]
        acc = None
        for bits in ((0, 1), (2, 3, 4, 5), (6,)):
            acc = product(out_weight, pieces(*bits), acc)
        out = store(part, out_weight, pieces(7), acc, out)
    return out


def solution(mesh):
    return jax.shard_map(
        shards,
        mesh=mesh,
        in_specs=(P("seq", None), P(), P(None, "tp"), P(None, "tp"), P(None, "tp"), P(None, "tp"), P()),
        out_specs=P("seq", "tp"),
        check_vma=False,
    )
```

```python
import functools
import math

import jax
import jax.numpy as jnp
import numpy as np
from jax import lax
from jax.experimental import pallas as pl
from jax.experimental.pallas import tpu as pltpu
from jax.sharding import PartitionSpec as P

HEAD_DIM = 128
WINDOW = 4096
EPSILON = 1e-05
BASE = 10000.0


VMEM = pl.BlockSpec(memory_space=pltpu.VMEM)
HBM = pl.BlockSpec(memory_space=pltpu.HBM)
PARAMS = pltpu.CompilerParams(vmem_limit_bytes=16 << 20)


def in_hbm(*arrays):
    return [pltpu.with_memory_space_constraint(a, pltpu.HBM) for a in arrays]


STEP = 16


def rotation_tables(block_rows, blocks):
    freqs = BASE ** (-2.0 * (np.arange(HEAD_DIM) % (HEAD_DIM // 2)) / HEAD_DIM)
    coarse = np.arange(0, block_rows * blocks, STEP)[:, None] * freqs
    fine = np.arange(STEP)[:, None] * freqs
    tables = (np.cos(coarse), np.sin(coarse), np.cos(fine), np.sin(fine))
    return [jnp.asarray(t, jnp.float32) for t in tables]


def rotate(x, cosine, sine):
    return (x * cosine + pltpu.roll(x, HEAD_DIM // 2, 1) * sine).astype(jnp.bfloat16)


def heads_of(width):
    return [slice(h, h + HEAD_DIM) for h in range(0, width, HEAD_DIM)]


def normalise(tokens, gain):
    wide = tokens.astype(jnp.float32)
    scale = lax.rsqrt(jnp.mean(wide * wide, axis=-1, keepdims=True) + EPSILON)
    return (wide * scale * gain).astype(jnp.bfloat16)


def key_value_of(normed, weight, cosine, sine, kv_ref, here):
    product = jnp.dot(normed, weight, preferred_element_type=jnp.float32)
    width = kv_ref.shape[1] // 2
    for h in heads_of(width):
        kv_ref[here, h] = rotate(product[:, h], cosine, sine)
    kv_ref[here, width:] = product[:, width:].astype(jnp.bfloat16)


def second_half_kernel(
    tile, tokens, gain, key_weight, value_weight, coarse_cos, coarse_sin, fine_cos, fine_sin, segments,
    kv_ref, normed_ref, weight, first_tokens, gain_copy, cosine, sine, limits,
    held, coarse_c, coarse_s, fine_c, fine_s, numbers, tile_sems, sems,
):
    rows, width = kv_ref.shape[0], key_weight.shape[1]
    steps = rows // tile
    tiles = [
        pltpu.make_async_copy(
            tokens.at[rows + i * tile : rows + (i + 1) * tile, :],
            held.at[i * tile : (i + 1) * tile, :],
            tile_sems.at[i],
        )
        for i in range(steps)
    ]
    groups = cosine.shape[0] // STEP
    coarse = pl.ds(pl.multiple_of(lax.axis_index("seq") * groups, groups), groups)
    moves = [
        (gain, gain_copy),
        (key_weight, weight.at[:, :width]),
        (value_weight, weight.at[:, width:]),
        (coarse_cos.at[coarse, :], coarse_c),
        (coarse_sin.at[coarse, :], coarse_s),
        (fine_cos, fine_c),
        (fine_sin, fine_s),
        (tokens.at[:rows, :], first_tokens),
        (segments, numbers),
    ]
    moves = [pltpu.make_async_copy(a, b, sems.at[i]) for i, (a, b) in enumerate(moves)]
    for move in [moves[8], moves[0]] + tiles[:2] + moves[3:7] + tiles[2:] + moves[1:3] + moves[7:8]:
        move.start()
    moves[8].wait()
    for value in (1, 2):
        before = jnp.sum((numbers[...] < value).astype(jnp.float32), axis=0, keepdims=True)
        count = jnp.broadcast_to(jnp.sum(before, axis=1, keepdims=True), before.shape)
        limits[value - 1 : value, :] = count.astype(jnp.int32)
    moves[0].wait()
    for i in range(steps):
        here = slice(i * tile, (i + 1) * tile)
        tiles[i].wait()
        normed_ref[here, :] = normalise(held[here, :], gain_copy[...])
    for move in moves[3:7]:
        move.wait()
    cos_f, sin_f = fine_c[...], fine_s[...]
    lane = lax.broadcasted_iota(jnp.int32, cos_f.shape, 1)
    for group in range(groups):
        cos_g, sin_g = coarse_c[group : group + 1, :], coarse_s[group : group + 1, :]
        turned = sin_g * cos_f + cos_g * sin_f
        here = slice(group * STEP, (group + 1) * STEP)
        cosine[here, :] = cos_g * cos_f - sin_g * sin_f
        sine[here, :] = jnp.where(lane < HEAD_DIM // 2, -turned, turned)
    moves[1].wait()
    moves[2].wait()
    key_value_of(normed_ref[...], weight[...], cosine[rows:, :], sine[rows:, :], kv_ref, slice(None))
    moves[7].wait()


def second_half(tokens, gain, key_weight, value_weight, tables, segments):
    block_rows, depth = tokens.shape
    half, width = block_rows // 2, key_weight.shape[1]
    tile = min(half, 32)
    shape, bf16, f32 = jax.ShapeDtypeStruct, jnp.bfloat16, jnp.float32
    return pl.pallas_call(
        functools.partial(second_half_kernel, tile),
        out_shape=(
            shape((half, 2 * width), bf16),
            shape((half, depth), bf16),
            shape((depth, 2 * width), bf16),
            shape((half, depth), bf16),
            shape(gain.shape, f32),
            shape((block_rows, HEAD_DIM), f32),
            shape((block_rows, HEAD_DIM), f32),
            shape((2, HEAD_DIM), jnp.int32),
        ),
        in_specs=[HBM] * 9,
        out_specs=(VMEM,) * 8,
        scratch_shapes=[pltpu.VMEM((half, depth), bf16)]
        + [pltpu.VMEM((block_rows // STEP, HEAD_DIM), f32)] * 2
        + [pltpu.VMEM((STEP, HEAD_DIM), f32)] * 2
        + [pltpu.VMEM(segments.shape, jnp.int32)]
        + [pltpu.SemaphoreType.DMA((half // tile,)), pltpu.SemaphoreType.DMA((9,))],
        compiler_params=PARAMS,
        name="second_half",
    )(*in_hbm(tokens, gain, key_weight, value_weight, *tables, segments))


def first_half_kernel(tokens, gain, weight, cosine, sine, kv_ref, normed_ref):
    rows = kv_ref.shape[0]
    normed_ref[...] = normalise(tokens[...], gain[...])
    key_value_of(normed_ref[...], weight[...], cosine[:rows, :], sine[:rows, :], kv_ref, slice(None))


def first_half(tokens, gain, weight, cosine, sine):
    half = tokens.shape[0]
    return pl.pallas_call(
        first_half_kernel,
        out_shape=(
            jax.ShapeDtypeStruct((half, weight.shape[1]), jnp.bfloat16),
            jax.ShapeDtypeStruct(tokens.shape, jnp.bfloat16),
        ),
        in_specs=[VMEM] * 5,
        out_specs=(VMEM,) * 2,
        compiler_params=PARAMS,
        name="first_half",
    )(tokens, gain, weight, cosine, sine)


def query_kernel(part, normed, weight, cosine, sine, out_ref):
    rows = slice(part * normed.shape[0], (part + 1) * normed.shape[0])
    product = jnp.dot(normed[...], weight[...], preferred_element_type=jnp.float32)
    for h in heads_of(weight.shape[1]):
        out_ref[:, h] = rotate(product[:, h], cosine[rows, :], sine[rows, :])


def query(part, normed, weight, cosine, sine):
    return pl.pallas_call(
        functools.partial(query_kernel, part),
        out_shape=jax.ShapeDtypeStruct((normed.shape[0], weight.shape[1]), jnp.bfloat16),
        in_specs=[VMEM] * 4,
        out_specs=VMEM,
        compiler_params=PARAMS,
    )(normed, weight, cosine, sine)


TILE, AHEAD = 256, 3
FACTOR = math.log2(math.e) / math.sqrt(HEAD_DIM)


def bias_of(part, place, back, half, limits, bias_ref, column):
    base = (2 * lax.axis_index("seq") + part) * half
    row = base + lax.broadcasted_iota(jnp.int32, (half, HEAD_DIM), 0)
    starts = [jnp.broadcast_to(limits[i : i + 1, :], row.shape) for i in range(2)]
    start = jnp.where(row >= starts[1], starts[1], jnp.where(row >= starts[0], starts[0], 0))
    start = jnp.maximum(start, row - (WINDOW - 1))
    first = base - (back - place) * half
    for left in range(0, half, HEAD_DIM):
        key = first + left + lax.broadcasted_iota(jnp.int32, (half, HEAD_DIM), 1)
        mask = key >= start
        if place == back:
            mask = mask & (key <= row)
        bias_ref[:, column + left : column + left + HEAD_DIM] = jnp.where(
            mask, jnp.float32(0), jnp.float32(-1e30)
        )


def attend_kernel(part, back, places, early, late, limits, q_ref, *refs):
    kv_refs, refs = refs[: len(places)], refs[len(places) :]
    bias_ref = refs[-1]
    half = q_ref.shape[0]
    kv_width = kv_refs[0].shape[1] // 2
    group = q_ref.shape[1] // kv_width
    for i, place in enumerate(places):
        bias_of(part, place, back, half, limits, bias_ref, i * half)
    ones = jnp.ones((half, HEAD_DIM), jnp.bfloat16)
    tile = min(half, TILE)
    wide = half // HEAD_DIM

    def score(h, rows):
        first = (h // group) * HEAD_DIM
        q = q_ref[rows, h * HEAD_DIM : (h + 1) * HEAD_DIM]
        scores = []
        for i, kv in enumerate(kv_refs):
            s = lax.dot_general(
                q, kv[:, first : first + HEAD_DIM], (((1,), (1,)), ((), ())), preferred_element_type=jnp.float32
            )
            scores.append(s * FACTOR + bias_ref[rows, i * half : (i + 1) * half])
        return scores

    def finish(h, rows, scores):
        first = kv_width + (h // group) * HEAD_DIM
        head = slice(h * HEAD_DIM, (h + 1) * HEAD_DIM)
        pair = slice(2 * h * HEAD_DIM, 2 * (h + 1) * HEAD_DIM)
        top = functools.reduce(jnp.maximum, scores)
        top = functools.reduce(jnp.maximum, [top[:, c * HEAD_DIM : (c + 1) * HEAD_DIM] for c in range(wide)])
        peak = jnp.broadcast_to(jnp.max(top, axis=-1, keepdims=True), top.shape)
        summed = 0.0
        if late:
            before = refs[1][rows, head]
            peak = jnp.maximum(peak, before)
            fade = jnp.exp2(before - peak)
            summed = refs[0][rows, pair] * jnp.concatenate([fade, fade], axis=1)
        peaks = jnp.concatenate([peak] * wide, axis=1)
        for s, kv in zip(scores, kv_refs):
            w = jnp.exp2(s - peaks).astype(jnp.bfloat16)
            both = jnp.concatenate([kv[:, first : first + HEAD_DIM], ones], axis=1)
            summed = summed + jnp.dot(w, both, preferred_element_type=jnp.float32)
        if early:
            refs[0][rows, pair] = summed
            refs[1][rows, head] = peak
        else:
            refs[-2][rows, head] = (summed[:, :HEAD_DIM] / summed[:, HEAD_DIM:]).astype(jnp.bfloat16)

    units = [
        (h, slice(row, row + tile)) for h in range(q_ref.shape[1] // HEAD_DIM) for row in range(0, half, tile)
    ]
    waiting = []
    for unit in units:
        waiting.append((*unit, score(*unit)))
        if len(waiting) > AHEAD:
            finish(*waiting.pop(0))
    for unit in waiting:
        finish(*unit)


def attend(part, back, places, queries, limits, key_values, early=False, before=()):
    half, width = queries.shape
    if early:
        shape = (
            jax.ShapeDtypeStruct((half, 2 * width), jnp.float32),
            jax.ShapeDtypeStruct((half, width), jnp.float32),
        )
    else:
        shape = jax.ShapeDtypeStruct((half, width), jnp.bfloat16)
    key_values = [key_values[p] for p in places]
    return pl.pallas_call(
        functools.partial(attend_kernel, part, back, tuple(places), early, bool(before)),
        out_shape=shape,
        in_specs=[VMEM] * (2 + len(places) + len(before)),
        out_specs=(VMEM, VMEM) if early else VMEM,
        scratch_shapes=[pltpu.VMEM((half, len(places) * half), jnp.float32)],
        compiler_params=pltpu.CompilerParams(vmem_limit_bytes=max(16, 2 * len(places)) << 20),
    )(limits, queries, *key_values, *before)


def added(bits, total, weight, xs):
    depth = xs[0].shape[1]
    me = lax.axis_index("tp")
    for bit, x in zip(bits, xs):
        owner = jnp.bitwise_xor(me, bit)
        rows = pl.ds(pl.multiple_of(owner * depth, depth), depth)
        total = total + jnp.dot(x[...], weight[rows, :], preferred_element_type=jnp.float32)
    return total


def product_kernel(bits, extra, weight, *refs):
    xs, out_ref = refs[: len(bits)], refs[-1]
    out_ref[...] = added(bits, refs[len(bits)][...] if extra else 0.0, weight, xs)


def product(weight, got, total=None):
    bits, xs = zip(*got)
    extra = () if total is None else (total,)
    return pl.pallas_call(
        functools.partial(product_kernel, bits, bool(extra)),
        out_shape=jax.ShapeDtypeStruct((xs[0].shape[0], weight.shape[1]), jnp.float32),
        in_specs=[VMEM] * (1 + len(xs) + len(extra)),
        out_specs=VMEM,
        compiler_params=PARAMS,
    )(weight, *xs, *extra)


def store_kernel(part, bits, weight, *refs):
    xs, total = refs[: len(bits)], refs[len(bits)]
    out_ref, rounded, sem = refs[-3:]
    rounded[...] = added(bits, total[...], weight, xs).astype(rounded.dtype)
    half = rounded.shape[0]
    move = pltpu.make_async_copy(rounded, out_ref.at[part * half : (part + 1) * half, :], sem)
    move.start()
    move.wait()


def store(part, weight, got, total, out=None):
    bits, xs = zip(*got)
    half, width = total.shape
    extra = () if out is None else in_hbm(out)
    count = 2 + len(xs)
    return pl.pallas_call(
        functools.partial(store_kernel, part, bits),
        out_shape=pltpu.HBM((2 * half, width), jnp.bfloat16),
        in_specs=[VMEM] * count + [HBM] * len(extra),
        out_specs=HBM,
        scratch_shapes=[pltpu.VMEM((half, width), jnp.bfloat16), pltpu.SemaphoreType.DMA],
        input_output_aliases={count: 0} if extra else {},
        compiler_params=PARAMS,
    )(weight, *xs, total, *extra)


def shards(tokens, norm_gain, query_weight, key_weight, value_weight, out_weight, segments):
    block_rows = tokens.shape[0]
    half = block_rows // 2
    seq_count, tp_count = lax.axis_size("seq"), lax.axis_size("tp")
    total = block_rows * seq_count
    reach = min(WINDOW, total // 2)
    back = min((reach - 2) // half + 1, 2 * seq_count - 1)

    def onward(hop):
        pairs = [(i, i + 1, 0) for i in range(hop - 1, seq_count - 1)]
        pairs = pairs + [(seq_count - 1, hop - 1, 0)] + [(i, i, 1) for i in range(hop - 1)]
        return [(a * tp_count + t, b * tp_count + (t ^ c)) for a, b, c in pairs for t in range(tp_count)]


    halves, normed, queries = [None] * (back + 2), [None, None], [None, None]
    halves[0], normed[1], weight, first_tokens, gain, cosine, sine, limits = second_half(
        tokens,
        norm_gain[None, :],
        key_weight,
        value_weight,
        rotation_tables(block_rows, seq_count),
        segments.reshape(-1, HEAD_DIM),
    )
    halves[1], normed[0] = first_half(first_tokens, gain, weight, cosine, sine)
    for distance in range(2, back + 2):
        halves[distance] = lax.ppermute(halves[distance - 2], ("seq", "tp"), onward(distance // 2))
    for part in (1, 0):
        queries[part] = query(part, normed[part], query_weight, cosine, sine)

    def swap(x, bit):
        return lax.ppermute(x, "tp", [(i, i ^ bit) for i in range(tp_count)])

    got, out = {}, None
    for part in (1, 0):
        key_values = halves[1 - part : 1 - part + back + 1][::-1]
        if part == 1:
            before = attend(part, back, range(1, back + 1), queries[part], limits, key_values, early=True)
            mine = attend(part, back, [0], queries[part], limits, key_values, before=before)
        else:
            mine = attend(part, back, range(back + 1), queries[part], limits, key_values)
        has = got[part] = {0: mine, 2: swap(mine, 2), 4: swap(mine, 4)}
        has[6] = swap(has[4], 2) if part == 0 else swap(has[2], 4)
        for bits in (0, 2, 4, 6):
            has[bits | 1] = swap(has[bits], 1)
    for part in (1, 0):
        pieces = lambda *bits: [(b, got[part][b]) for b in bits]
        acc = None
        for bits in ((0, 1), (2, 3, 4, 5), (6,)):
            acc = product(out_weight, pieces(*bits), acc)
        out = store(part, out_weight, pieces(7), acc, out)
    return out


def solution(mesh):
    return jax.shard_map(
        shards,
        mesh=mesh,
        in_specs=(P("seq", None), P(), P(None, "tp"), P(None, "tp"), P(None, "tp"), P(None, "tp"), P()),
        out_specs=P("seq", "tp"),
        check_vma=False,
    )
```

```python
import functools
import math

import jax
import jax.numpy as jnp
import numpy as np
from jax import lax
from jax.experimental import pallas as pl
from jax.experimental.pallas import tpu as pltpu
from jax.sharding import PartitionSpec as P

HEAD_DIM = 128
WINDOW = 4096
EPSILON = 1e-05
BASE = 10000.0


VMEM = pl.BlockSpec(memory_space=pltpu.VMEM)
HBM = pl.BlockSpec(memory_space=pltpu.HBM)
PARAMS = pltpu.CompilerParams(vmem_limit_bytes=16 << 20)


def in_hbm(*arrays):
    return [pltpu.with_memory_space_constraint(a, pltpu.HBM) for a in arrays]


STEP = 16


def rotation_tables(block_rows, blocks):
    freqs = BASE ** (-2.0 * (np.arange(HEAD_DIM) % (HEAD_DIM // 2)) / HEAD_DIM)
    coarse = np.arange(0, block_rows * blocks, STEP)[:, None] * freqs
    fine = np.arange(STEP)[:, None] * freqs
    tables = (np.cos(coarse), np.sin(coarse), np.cos(fine), np.sin(fine))
    return [jnp.asarray(t, jnp.float32) for t in tables]


def rotate(x, cosine, sine):
    return (x * cosine + pltpu.roll(x, HEAD_DIM // 2, 1) * sine).astype(jnp.bfloat16)


def heads_of(width):
    return [slice(h, h + HEAD_DIM) for h in range(0, width, HEAD_DIM)]


def normalise(tokens, gain):
    wide = tokens.astype(jnp.float32)
    scale = lax.rsqrt(jnp.mean(wide * wide, axis=-1, keepdims=True) + EPSILON)
    return (wide * scale * gain).astype(jnp.bfloat16)


def key_value_of(normed, weight, cosine, sine, kv_ref, here):
    product = jnp.dot(normed, weight, preferred_element_type=jnp.float32)
    width = kv_ref.shape[1] // 2
    for h in heads_of(width):
        kv_ref[here, h] = rotate(product[:, h], cosine, sine)
    kv_ref[here, width:] = product[:, width:].astype(jnp.bfloat16)


def second_half_kernel(
    tile, tokens, gain, key_weight, value_weight, coarse_cos, coarse_sin, fine_cos, fine_sin, segments,
    kv_ref, normed_ref, weight, first_tokens, gain_copy, cosine, sine, limits,
    held, coarse_c, coarse_s, fine_c, fine_s, numbers, tile_sems, sems,
):
    rows, width = kv_ref.shape[0], key_weight.shape[1]
    steps = rows // tile
    tiles = [
        pltpu.make_async_copy(
            tokens.at[rows + i * tile : rows + (i + 1) * tile, :],
            held.at[i * tile : (i + 1) * tile, :],
            tile_sems.at[i],
        )
        for i in range(steps)
    ]
    groups = cosine.shape[0] // STEP
    coarse = pl.ds(pl.multiple_of(lax.axis_index("seq") * groups, groups), groups)
    moves = [
        (gain, gain_copy),
        (key_weight, weight.at[:, :width]),
        (value_weight, weight.at[:, width:]),
        (coarse_cos.at[coarse, :], coarse_c),
        (coarse_sin.at[coarse, :], coarse_s),
        (fine_cos, fine_c),
        (fine_sin, fine_s),
        (tokens.at[:rows, :], first_tokens),
        (segments, numbers),
    ]
    moves = [pltpu.make_async_copy(a, b, sems.at[i]) for i, (a, b) in enumerate(moves)]
    for move in [moves[8], moves[0]] + tiles[:2] + moves[3:7] + tiles[2:] + moves[1:3] + moves[7:8]:
        move.start()
    moves[8].wait()
    for value in (1, 2):
        before = jnp.sum((numbers[...] < value).astype(jnp.float32), axis=0, keepdims=True)
        count = jnp.broadcast_to(jnp.sum(before, axis=1, keepdims=True), before.shape)
        limits[value - 1 : value, :] = count.astype(jnp.int32)
    moves[0].wait()
    for i in range(steps):
        here = slice(i * tile, (i + 1) * tile)
        tiles[i].wait()
        normed_ref[here, :] = normalise(held[here, :], gain_copy[...])
    for move in moves[3:7]:
        move.wait()
    cos_f, sin_f = fine_c[...], fine_s[...]
    lane = lax.broadcasted_iota(jnp.int32, cos_f.shape, 1)
    for group in range(groups):
        cos_g, sin_g = coarse_c[group : group + 1, :], coarse_s[group : group + 1, :]
        turned = sin_g * cos_f + cos_g * sin_f
        here = slice(group * STEP, (group + 1) * STEP)
        cosine[here, :] = cos_g * cos_f - sin_g * sin_f
        sine[here, :] = jnp.where(lane < HEAD_DIM // 2, -turned, turned)
    moves[1].wait()
    moves[2].wait()
    key_value_of(normed_ref[...], weight[...], cosine[rows:, :], sine[rows:, :], kv_ref, slice(None))
    moves[7].wait()


def second_half(tokens, gain, key_weight, value_weight, tables, segments):
    block_rows, depth = tokens.shape
    half, width = block_rows // 2, key_weight.shape[1]
    tile = min(half, 32)
    shape, bf16, f32 = jax.ShapeDtypeStruct, jnp.bfloat16, jnp.float32
    return pl.pallas_call(
        functools.partial(second_half_kernel, tile),
        out_shape=(
            shape((half, 2 * width), bf16),
            shape((half, depth), bf16),
            shape((depth, 2 * width), bf16),
            shape((half, depth), bf16),
            shape(gain.shape, f32),
            shape((block_rows, HEAD_DIM), f32),
            shape((block_rows, HEAD_DIM), f32),
            shape((2, HEAD_DIM), jnp.int32),
        ),
        in_specs=[HBM] * 9,
        out_specs=(VMEM,) * 8,
        scratch_shapes=[pltpu.VMEM((half, depth), bf16)]
        + [pltpu.VMEM((block_rows // STEP, HEAD_DIM), f32)] * 2
        + [pltpu.VMEM((STEP, HEAD_DIM), f32)] * 2
        + [pltpu.VMEM(segments.shape, jnp.int32)]
        + [pltpu.SemaphoreType.DMA((half // tile,)), pltpu.SemaphoreType.DMA((9,))],
        compiler_params=PARAMS,
        name="second_half",
    )(*in_hbm(tokens, gain, key_weight, value_weight, *tables, segments))


def first_half_kernel(tokens, gain, weight, cosine, sine, kv_ref, normed_ref):
    rows = kv_ref.shape[0]
    normed_ref[...] = normalise(tokens[...], gain[...])
    key_value_of(normed_ref[...], weight[...], cosine[:rows, :], sine[:rows, :], kv_ref, slice(None))


def first_half(tokens, gain, weight, cosine, sine):
    half = tokens.shape[0]
    return pl.pallas_call(
        first_half_kernel,
        out_shape=(
            jax.ShapeDtypeStruct((half, weight.shape[1]), jnp.bfloat16),
            jax.ShapeDtypeStruct(tokens.shape, jnp.bfloat16),
        ),
        in_specs=[VMEM] * 5,
        out_specs=(VMEM,) * 2,
        compiler_params=PARAMS,
        name="first_half",
    )(tokens, gain, weight, cosine, sine)


def query_kernel(part, normed, weight, cosine, sine, out_ref):
    rows = slice(part * normed.shape[0], (part + 1) * normed.shape[0])
    product = jnp.dot(normed[...], weight[...], preferred_element_type=jnp.float32)
    for h in heads_of(weight.shape[1]):
        out_ref[:, h] = rotate(product[:, h], cosine[rows, :], sine[rows, :])


def query(part, normed, weight, cosine, sine):
    return pl.pallas_call(
        functools.partial(query_kernel, part),
        out_shape=jax.ShapeDtypeStruct((normed.shape[0], weight.shape[1]), jnp.bfloat16),
        in_specs=[VMEM] * 4,
        out_specs=VMEM,
        compiler_params=PARAMS,
    )(normed, weight, cosine, sine)


AHEAD = 3
FACTOR = math.log2(math.e) / math.sqrt(HEAD_DIM)


def bias_of(part, place, back, half, limits, bias_ref, column):
    base = (2 * lax.axis_index("seq") + part) * half
    row = base + lax.broadcasted_iota(jnp.int32, (half, HEAD_DIM), 0)
    starts = [jnp.broadcast_to(limits[i : i + 1, :], row.shape) for i in range(2)]
    start = jnp.where(row >= starts[1], starts[1], jnp.where(row >= starts[0], starts[0], 0))
    start = jnp.maximum(start, row - (WINDOW - 1))
    first = base - (back - place) * half
    for left in range(0, half, HEAD_DIM):
        key = first + left + lax.broadcasted_iota(jnp.int32, (half, HEAD_DIM), 1)
        mask = key >= start
        if place == back:
            mask = mask & (key <= row)
        bias_ref[:, column + left : column + left + HEAD_DIM] = jnp.where(
            mask, jnp.float32(0), jnp.float32(-1e30)
        )


def attend_kernel(part, back, places, early, late, limits, q_ref, *refs):
    kv_refs, refs = refs[: len(places)], refs[len(places) :]
    bias_ref = refs[-1]
    outs = 2 if late else 0
    half = q_ref.shape[0]
    kv_width = kv_refs[0].shape[1] // 2
    group = q_ref.shape[1] // kv_width
    for i, place in enumerate(places):
        bias_of(part, place, back, half, limits, bias_ref, i * half)
    ones = jnp.ones((half, HEAD_DIM), jnp.bfloat16)
    tile = half
    wide = half // HEAD_DIM

    def score(h, rows):
        first = (h // group) * HEAD_DIM
        q = q_ref[rows, h * HEAD_DIM : (h + 1) * HEAD_DIM]
        scores = []
        for i, kv in enumerate(kv_refs):
            s = lax.dot_general(
                q, kv[:, first : first + HEAD_DIM], (((1,), (1,)), ((), ())), preferred_element_type=jnp.float32
            )
            scores.append(s * FACTOR + bias_ref[rows, i * half : (i + 1) * half])
        return scores

    def finish(h, rows, scores):
        first = kv_width + (h // group) * HEAD_DIM
        head = slice(h * HEAD_DIM, (h + 1) * HEAD_DIM)
        pair = slice(2 * h * HEAD_DIM, 2 * (h + 1) * HEAD_DIM)
        top = functools.reduce(jnp.maximum, scores)
        top = functools.reduce(jnp.maximum, [top[:, c * HEAD_DIM : (c + 1) * HEAD_DIM] for c in range(wide)])
        peak = jnp.broadcast_to(jnp.max(top, axis=-1, keepdims=True), top.shape)
        summed = 0.0
        if late:
            before = refs[1][rows, head]
            peak = jnp.maximum(peak, before)
            fade = jnp.exp2(before - peak)
            summed = refs[0][rows, pair] * jnp.concatenate([fade, fade], axis=1)
        peaks = jnp.concatenate([peak] * wide, axis=1)
        for s, kv in zip(scores, kv_refs):
            w = jnp.exp2(s - peaks).astype(jnp.bfloat16)
            both = jnp.concatenate([kv[:, first : first + HEAD_DIM], ones], axis=1)
            summed = summed + jnp.dot(w, both, preferred_element_type=jnp.float32)
        if early:
            refs[0][rows, pair] = summed
            refs[1][rows, head] = peak
        else:
            result = (summed[:, :HEAD_DIM] / summed[:, HEAD_DIM:]).astype(jnp.bfloat16)
            refs[outs][rows, head] = result
            for i, piece in enumerate(refs[outs + 1 : -1]):
                piece[:, head] = result[i * piece.shape[0] : (i + 1) * piece.shape[0], :]

    units = [
        (h, slice(row, row + tile)) for h in range(q_ref.shape[1] // HEAD_DIM) for row in range(0, half, tile)
    ]
    waiting = []
    for unit in units:
        waiting.append((*unit, score(*unit)))
        if len(waiting) > AHEAD:
            finish(*waiting.pop(0))
    for unit in waiting:
        finish(*unit)


def attend(part, back, places, queries, limits, key_values, early=False, before=(), pieces=0):
    half, width = queries.shape
    if early:
        shape = (
            jax.ShapeDtypeStruct((half, 2 * width), jnp.float32),
            jax.ShapeDtypeStruct((half, width), jnp.float32),
        )
    else:
        shape = [jax.ShapeDtypeStruct((half, width), jnp.bfloat16)]
        shape += [jax.ShapeDtypeStruct((half // max(pieces, 1), width), jnp.bfloat16)] * pieces
    key_values = [key_values[p] for p in places]
    return pl.pallas_call(
        functools.partial(attend_kernel, part, back, tuple(places), early, bool(before)),
        out_shape=shape,
        in_specs=[VMEM] * (2 + len(places) + len(before)),
        out_specs=[VMEM] * len(shape),
        scratch_shapes=[pltpu.VMEM((half, len(places) * half), jnp.float32)],
        compiler_params=pltpu.CompilerParams(vmem_limit_bytes=max(16, 2 * len(places)) << 20),
    )(limits, queries, *key_values, *before)


def added(bits, total, weight, pieces):
    depth = pieces[0][0].shape[1]
    me = lax.axis_index("tp")
    for bit, piece in zip(bits, pieces):
        owner = jnp.bitwise_xor(me, bit)
        rows = pl.ds(pl.multiple_of(owner * depth, depth), depth)
        x = jnp.concatenate([a[...] for a in piece], axis=0) if len(piece) > 1 else piece[0][...]
        total = total + jnp.dot(x, weight[rows, :], preferred_element_type=jnp.float32)
    return total


def grouped(refs, counts):
    groups, place = [], 0
    for count in counts:
        groups.append(refs[place : place + count])
        place += count
    return groups, refs[place:]


def product_kernel(bits, counts, weight, *refs):
    pieces, rest = grouped(refs, counts)
    rest[-1][...] = added(bits, rest[0][...] if len(rest) > 1 else 0.0, weight, pieces)


def product(weight, got, total=None):
    bits, pieces = zip(*got)
    counts = [len(piece) for piece in pieces]
    xs = [a for piece in pieces for a in piece]
    extra = () if total is None else (total,)
    return pl.pallas_call(
        functools.partial(product_kernel, bits, counts),
        out_shape=jax.ShapeDtypeStruct((sum(a.shape[0] for a in pieces[0]), weight.shape[1]), jnp.float32),
        in_specs=[VMEM] * (1 + len(xs) + len(extra)),
        out_specs=VMEM,
        compiler_params=PARAMS,
    )(weight, *xs, *extra)


def store_kernel(bits, counts, weight, *refs):
    pieces, rest = grouped(refs, counts)
    totals, (out_ref, rounded, sems) = rest[:2], rest[2:]
    half = totals[0].shape[0]
    moves = []
    for part in (1, 0):
        rows = slice(part * half, (part + 1) * half)
        rounded[rows, :] = added(bits[part], totals[part][...], weight, [pieces[part]]).astype(rounded.dtype)
        moves.append(pltpu.make_async_copy(rounded.at[rows, :], out_ref.at[rows, :], sems.at[part]))
        moves[-1].start()
    for move in moves:
        move.wait()


def store(weight, bits, pieces, totals):
    xs = [a for piece in pieces for a in piece]
    half, width = totals[0].shape
    return pl.pallas_call(
        functools.partial(store_kernel, [(bits,)] * 2, [len(piece) for piece in pieces]),
        out_shape=pltpu.HBM((2 * half, width), jnp.bfloat16),
        in_specs=[VMEM] * (3 + len(xs)),
        out_specs=HBM,
        scratch_shapes=[pltpu.VMEM((2 * half, width), jnp.bfloat16), pltpu.SemaphoreType.DMA((2,))],
        compiler_params=PARAMS,
        name="store",
    )(weight, *xs, *totals)


def shards(tokens, norm_gain, query_weight, key_weight, value_weight, out_weight, segments):
    block_rows = tokens.shape[0]
    half = block_rows // 2
    seq_count, tp_count = lax.axis_size("seq"), lax.axis_size("tp")
    total = block_rows * seq_count
    reach = min(WINDOW, total // 2)
    back = min((reach - 2) // half + 1, 2 * seq_count - 1)

    def onward(hop):
        pairs = [(i, i + 1, 0) for i in range(hop - 1, seq_count - 1)]
        pairs = pairs + [(seq_count - 1, hop - 1, 0)] + [(i, i, 1) for i in range(hop - 1)]
        return [(a * tp_count + t, b * tp_count + (t ^ c)) for a, b, c in pairs for t in range(tp_count)]


    halves, normed, queries = [None] * (back + 2), [None, None], [None, None]
    halves[0], normed[1], weight, first_tokens, gain, cosine, sine, limits = second_half(
        tokens,
        norm_gain[None, :],
        key_weight,
        value_weight,
        rotation_tables(block_rows, seq_count),
        segments.reshape(-1, HEAD_DIM),
    )
    halves[1], normed[0] = first_half(first_tokens, gain, weight, cosine, sine)
    for distance in range(2, back + 2):
        halves[distance] = lax.ppermute(halves[distance - 2], ("seq", "tp"), onward(distance // 2))
    for part in (1, 0):
        queries[part] = query(part, normed[part], query_weight, cosine, sine)

    def swap(x, bit):
        return lax.ppermute(x, "tp", [(i, i ^ bit) for i in range(tp_count)])

    got, totals = {}, [None, None]
    for part in (1, 0):
        key_values = halves[1 - part : 1 - part + back + 1][::-1]
        if part == 1:
            before = attend(part, back, range(back - 2, back + 1), queries[part], limits, key_values, early=True)
            (mine,) = attend(part, back, range(back - 2), queries[part], limits, key_values, before=before)
        else:
            mine, *pair = attend(part, back, range(back + 1), queries[part], limits, key_values, pieces=2)
        if part == 1:
            x, y = swap(mine, 2), swap(mine, 4)
            has = {0: (mine,), 2: (x,), 4: (y,), 6: (swap(x, 4),)}
        else:
            y = [swap(a, 4) for a in pair]
            x = swap(mine, 2)
            has = {0: (mine,), 2: (x,), 4: tuple(y), 6: tuple(swap(a, 2) for a in y)}
        for bits in (0, 2, 4, 6):
            has[bits | 1] = tuple(swap(a, 1) for a in has[bits])
        got[part] = has
    for part in (1, 0):
        pieces = lambda *bits: [(b, got[part][b]) for b in bits]
        acc = None
        for bits in ((0, 1), (2, 3, 4, 5), (6,)):
            acc = product(out_weight, pieces(*bits), acc)
        totals[part] = acc
    return store(out_weight, 7, [got[part][7] for part in (0, 1)], totals)


def solution(mesh):
    return jax.shard_map(
        shards,
        mesh=mesh,
        in_specs=(P("seq", None), P(), P(None, "tp"), P(None, "tp"), P(None, "tp"), P(None, "tp"), P()),
        out_specs=P("seq", "tp"),
        check_vma=False,
    )
```

```python
import functools
import math

import jax
import jax.numpy as jnp
import numpy as np
from jax import lax
from jax.experimental import pallas as pl
from jax.experimental.pallas import tpu as pltpu
from jax.sharding import PartitionSpec as P

HEAD_DIM = 128
WINDOW = 4096
EPSILON = 1e-05
BASE = 10000.0


VMEM = pl.BlockSpec(memory_space=pltpu.VMEM)
HBM = pl.BlockSpec(memory_space=pltpu.HBM)
PARAMS = pltpu.CompilerParams(vmem_limit_bytes=16 << 20)


def in_hbm(*arrays):
    return [pltpu.with_memory_space_constraint(a, pltpu.HBM) for a in arrays]


STEP = 16


def rotation_tables(block_rows, blocks):
    freqs = BASE ** (-2.0 * (np.arange(HEAD_DIM) % (HEAD_DIM // 2)) / HEAD_DIM)
    coarse = np.arange(0, block_rows * blocks, STEP)[:, None] * freqs
    fine = np.arange(STEP)[:, None] * freqs
    tables = (np.cos(coarse), np.sin(coarse), np.cos(fine), np.sin(fine))
    return [jnp.asarray(t, jnp.float32) for t in tables]


def rotate(x, cosine, sine):
    return (x * cosine + pltpu.roll(x, HEAD_DIM // 2, 1) * sine).astype(jnp.bfloat16)


def heads_of(width):
    return [slice(h, h + HEAD_DIM) for h in range(0, width, HEAD_DIM)]


def normalise(tokens, gain):
    wide = tokens.astype(jnp.float32)
    scale = lax.rsqrt(jnp.mean(wide * wide, axis=-1, keepdims=True) + EPSILON)
    return (wide * scale * gain).astype(jnp.bfloat16)


def key_value_of(normed, weight, cosine, sine, kv_ref, here):
    product = jnp.dot(normed, weight, preferred_element_type=jnp.float32)
    width = kv_ref.shape[1] // 2
    for h in heads_of(width):
        kv_ref[here, h] = rotate(product[:, h], cosine, sine)
    kv_ref[here, width:] = product[:, width:].astype(jnp.bfloat16)


def second_half_kernel(
    tile, tokens, gain, key_weight, value_weight, coarse_cos, coarse_sin, fine_cos, fine_sin, segments,
    kv_ref, normed_ref, weight, first_tokens, gain_copy, cosine, sine, limits,
    held, coarse_c, coarse_s, fine_c, fine_s, numbers, tile_sems, sems,
):
    rows, width = kv_ref.shape[0], key_weight.shape[1]
    steps = rows // tile
    tiles = [
        pltpu.make_async_copy(
            tokens.at[rows + i * tile : rows + (i + 1) * tile, :],
            held.at[i * tile : (i + 1) * tile, :],
            tile_sems.at[i],
        )
        for i in range(steps)
    ]
    groups = cosine.shape[0] // STEP
    coarse = pl.ds(pl.multiple_of(lax.axis_index("seq") * groups, groups), groups)
    moves = [
        (gain, gain_copy),
        (key_weight, weight.at[:, :width]),
        (value_weight, weight.at[:, width:]),
        (coarse_cos.at[coarse, :], coarse_c),
        (coarse_sin.at[coarse, :], coarse_s),
        (fine_cos, fine_c),
        (fine_sin, fine_s),
        (tokens.at[:rows, :], first_tokens),
        (segments, numbers),
    ]
    moves = [pltpu.make_async_copy(a, b, sems.at[i]) for i, (a, b) in enumerate(moves)]
    for move in [moves[8], moves[0]] + tiles[:2] + moves[3:7] + tiles[2:] + moves[1:3] + moves[7:8]:
        move.start()
    moves[8].wait()
    for value in (1, 2):
        before = jnp.sum((numbers[...] < value).astype(jnp.float32), axis=0, keepdims=True)
        count = jnp.broadcast_to(jnp.sum(before, axis=1, keepdims=True), before.shape)
        limits[value - 1 : value, :] = count.astype(jnp.int32)
    moves[0].wait()
    for i in range(steps):
        here = slice(i * tile, (i + 1) * tile)
        tiles[i].wait()
        normed_ref[here, :] = normalise(held[here, :], gain_copy[...])
    for move in moves[3:7]:
        move.wait()
    cos_f, sin_f = fine_c[...], fine_s[...]
    lane = lax.broadcasted_iota(jnp.int32, cos_f.shape, 1)
    for group in range(groups):
        cos_g, sin_g = coarse_c[group : group + 1, :], coarse_s[group : group + 1, :]
        turned = sin_g * cos_f + cos_g * sin_f
        here = slice(group * STEP, (group + 1) * STEP)
        cosine[here, :] = cos_g * cos_f - sin_g * sin_f
        sine[here, :] = jnp.where(lane < HEAD_DIM // 2, -turned, turned)
    moves[1].wait()
    moves[2].wait()
    key_value_of(normed_ref[...], weight[...], cosine[rows:, :], sine[rows:, :], kv_ref, slice(None))
    moves[7].wait()


def second_half(tokens, gain, key_weight, value_weight, tables, segments):
    block_rows, depth = tokens.shape
    half, width = block_rows // 2, key_weight.shape[1]
    tile = min(half, 32)
    shape, bf16, f32 = jax.ShapeDtypeStruct, jnp.bfloat16, jnp.float32
    return pl.pallas_call(
        functools.partial(second_half_kernel, tile),
        out_shape=(
            shape((half, 2 * width), bf16),
            shape((half, depth), bf16),
            shape((depth, 2 * width), bf16),
            shape((half, depth), bf16),
            shape(gain.shape, f32),
            shape((block_rows, HEAD_DIM), f32),
            shape((block_rows, HEAD_DIM), f32),
            shape((2, HEAD_DIM), jnp.int32),
        ),
        in_specs=[HBM] * 9,
        out_specs=(VMEM,) * 8,
        scratch_shapes=[pltpu.VMEM((half, depth), bf16)]
        + [pltpu.VMEM((block_rows // STEP, HEAD_DIM), f32)] * 2
        + [pltpu.VMEM((STEP, HEAD_DIM), f32)] * 2
        + [pltpu.VMEM(segments.shape, jnp.int32)]
        + [pltpu.SemaphoreType.DMA((half // tile,)), pltpu.SemaphoreType.DMA((9,))],
        compiler_params=PARAMS,
        name="second_half",
    )(*in_hbm(tokens, gain, key_weight, value_weight, *tables, segments))


def first_half_kernel(tokens, gain, weight, cosine, sine, kv_ref, normed_ref):
    rows = kv_ref.shape[0]
    normed_ref[...] = normalise(tokens[...], gain[...])
    key_value_of(normed_ref[...], weight[...], cosine[:rows, :], sine[:rows, :], kv_ref, slice(None))


def first_half(tokens, gain, weight, cosine, sine):
    half = tokens.shape[0]
    return pl.pallas_call(
        first_half_kernel,
        out_shape=(
            jax.ShapeDtypeStruct((half, weight.shape[1]), jnp.bfloat16),
            jax.ShapeDtypeStruct(tokens.shape, jnp.bfloat16),
        ),
        in_specs=[VMEM] * 5,
        out_specs=(VMEM,) * 2,
        compiler_params=PARAMS,
        name="first_half",
    )(tokens, gain, weight, cosine, sine)


def query_kernel(part, normed, weight, cosine, sine, out_ref):
    rows = slice(part * normed.shape[0], (part + 1) * normed.shape[0])
    product = jnp.dot(normed[...], weight[...], preferred_element_type=jnp.float32)
    for h in heads_of(weight.shape[1]):
        out_ref[:, h] = rotate(product[:, h], cosine[rows, :], sine[rows, :])


def query(part, normed, weight, cosine, sine):
    return pl.pallas_call(
        functools.partial(query_kernel, part),
        out_shape=jax.ShapeDtypeStruct((normed.shape[0], weight.shape[1]), jnp.bfloat16),
        in_specs=[VMEM] * 4,
        out_specs=VMEM,
        compiler_params=PARAMS,
    )(normed, weight, cosine, sine)


AHEAD = 3
FACTOR = math.log2(math.e) / math.sqrt(HEAD_DIM)


def bias_of(part, place, back, half, limits, bias_ref, column):
    base = (2 * lax.axis_index("seq") + part) * half
    row = base + lax.broadcasted_iota(jnp.int32, (half, HEAD_DIM), 0)
    starts = [jnp.broadcast_to(limits[i : i + 1, :], row.shape) for i in range(2)]
    start = jnp.where(row >= starts[1], starts[1], jnp.where(row >= starts[0], starts[0], 0))
    start = jnp.maximum(start, row - (WINDOW - 1))
    first = base - (back - place) * half
    for left in range(0, half, HEAD_DIM):
        key = first + left + lax.broadcasted_iota(jnp.int32, (half, HEAD_DIM), 1)
        mask = key >= start
        if place == back:
            mask = mask & (key <= row)
        bias_ref[:, column + left : column + left + HEAD_DIM] = jnp.where(
            mask, jnp.float32(0), jnp.float32(-1e30)
        )


def attend_kernel(part, back, places, early, late, limits, q_ref, *refs):
    kv_refs, refs = refs[: len(places)], refs[len(places) :]
    bias_ref = refs[-1]
    outs = 2 if late else 0
    half = q_ref.shape[0]
    kv_width = kv_refs[0].shape[1] // 2
    group = q_ref.shape[1] // kv_width
    for i, place in enumerate(places):
        bias_of(part, place, back, half, limits, bias_ref, i * half)
    ones = jnp.ones((half, HEAD_DIM), jnp.bfloat16)
    tile = half
    wide = half // HEAD_DIM

    def score(h, rows):
        first = (h // group) * HEAD_DIM
        q = q_ref[rows, h * HEAD_DIM : (h + 1) * HEAD_DIM]
        scores = []
        for i, kv in enumerate(kv_refs):
            s = lax.dot_general(
                q, kv[:, first : first + HEAD_DIM], (((1,), (1,)), ((), ())), preferred_element_type=jnp.float32
            )
            scores.append(s * FACTOR + bias_ref[rows, i * half : (i + 1) * half])
        return scores

    def finish(h, rows, scores):
        first = kv_width + (h // group) * HEAD_DIM
        head = slice(h * HEAD_DIM, (h + 1) * HEAD_DIM)
        pair = slice(2 * h * HEAD_DIM, 2 * (h + 1) * HEAD_DIM)
        top = functools.reduce(jnp.maximum, scores)
        top = functools.reduce(jnp.maximum, [top[:, c * HEAD_DIM : (c + 1) * HEAD_DIM] for c in range(wide)])
        peak = jnp.broadcast_to(jnp.max(top, axis=-1, keepdims=True), top.shape)
        summed = 0.0
        if late:
            before = refs[1][rows, head]
            peak = jnp.maximum(peak, before)
            fade = jnp.exp2(before - peak)
            summed = refs[0][rows, pair] * jnp.concatenate([fade, fade], axis=1)
        peaks = jnp.concatenate([peak] * wide, axis=1)
        for s, kv in zip(scores, kv_refs):
            w = jnp.exp2(s - peaks).astype(jnp.bfloat16)
            both = jnp.concatenate([kv[:, first : first + HEAD_DIM], ones], axis=1)
            summed = summed + jnp.dot(w, both, preferred_element_type=jnp.float32)
        if early:
            refs[0][rows, pair] = summed
            refs[1][rows, head] = peak
        else:
            result = (summed[:, :HEAD_DIM] / summed[:, HEAD_DIM:]).astype(jnp.bfloat16)
            refs[outs][rows, head] = result
            for i, piece in enumerate(refs[outs + 1 : -1]):
                piece[:, head] = result[i * piece.shape[0] : (i + 1) * piece.shape[0], :]

    units = [
        (h, slice(row, row + tile)) for h in range(q_ref.shape[1] // HEAD_DIM) for row in range(0, half, tile)
    ]
    waiting = []
    for unit in units:
        waiting.append((*unit, score(*unit)))
        if len(waiting) > AHEAD:
            finish(*waiting.pop(0))
    for unit in waiting:
        finish(*unit)


def attend(part, back, places, queries, limits, key_values, early=False, before=(), pieces=0):
    half, width = queries.shape
    if early:
        shape = (
            jax.ShapeDtypeStruct((half, 2 * width), jnp.float32),
            jax.ShapeDtypeStruct((half, width), jnp.float32),
        )
    else:
        shape = [jax.ShapeDtypeStruct((half, width), jnp.bfloat16)]
        shape += [jax.ShapeDtypeStruct((half // max(pieces, 1), width), jnp.bfloat16)] * pieces
    key_values = [key_values[p] for p in places]
    return pl.pallas_call(
        functools.partial(attend_kernel, part, back, tuple(places), early, bool(before)),
        out_shape=shape,
        in_specs=[VMEM] * (2 + len(places) + len(before)),
        out_specs=[VMEM] * len(shape),
        scratch_shapes=[pltpu.VMEM((half, len(places) * half), jnp.float32)],
        compiler_params=pltpu.CompilerParams(vmem_limit_bytes=max(16, 2 * len(places)) << 20),
    )(limits, queries, *key_values, *before)


def added(bits, total, weight, pieces):
    me = lax.axis_index("tp")
    for bit, piece in zip(bits, pieces):
        depth = piece[0].shape[1]
        owner = jnp.bitwise_xor(me, bit)
        rows = pl.ds(pl.multiple_of(owner * depth, depth), depth)
        x = jnp.concatenate([a[...] for a in piece], axis=0) if len(piece) > 1 else piece[0][...]
        total = total + jnp.dot(x, weight[rows, :], preferred_element_type=jnp.float32)
    return total


def grouped(refs, counts):
    groups, place = [], 0
    for count in counts:
        groups.append(refs[place : place + count])
        place += count
    return groups, refs[place:]


def product_kernel(bits, counts, weight, *refs):
    pieces, rest = grouped(refs, counts)
    rest[-1][...] = added(bits, rest[0][...] if len(rest) > 1 else 0.0, weight, pieces)


def product(weight, got, total=None):
    bits, pieces = zip(*got)
    counts = [len(piece) for piece in pieces]
    xs = [a for piece in pieces for a in piece]
    extra = () if total is None else (total,)
    return pl.pallas_call(
        functools.partial(product_kernel, bits, counts),
        out_shape=jax.ShapeDtypeStruct((sum(a.shape[0] for a in pieces[0]), weight.shape[1]), jnp.float32),
        in_specs=[VMEM] * (1 + len(xs) + len(extra)),
        out_specs=VMEM,
        compiler_params=PARAMS,
    )(weight, *xs, *extra)


def store_kernel(bits, counts, weight, *refs):
    pieces, rest = grouped(refs, counts)
    totals, (out_ref, rounded, sems) = rest[:2], rest[2:]
    half = totals[0].shape[0]
    moves = []
    for part in (1, 0):
        rows = slice(part * half, (part + 1) * half)
        rounded[rows, :] = added(bits[part], totals[part][...], weight, pieces[part : part + 1]).astype(rounded.dtype)
        moves.append(pltpu.make_async_copy(rounded.at[rows, :], out_ref.at[rows, :], sems.at[part]))
        moves[-1].start()
    for move in moves:
        move.wait()


def store(weight, bits, pieces, totals):
    xs = [a for piece in pieces for a in piece]
    half, width = totals[0].shape
    return pl.pallas_call(
        functools.partial(store_kernel, [(bits,), ()], [len(piece) for piece in pieces]),
        out_shape=pltpu.HBM((2 * half, width), jnp.bfloat16),
        in_specs=[VMEM] * (3 + len(xs)),
        out_specs=HBM,
        scratch_shapes=[pltpu.VMEM((2 * half, width), jnp.bfloat16), pltpu.SemaphoreType.DMA((2,))],
        compiler_params=PARAMS,
        name="store",
    )(weight, *xs, *totals)


def shards(tokens, norm_gain, query_weight, key_weight, value_weight, out_weight, segments):
    block_rows = tokens.shape[0]
    half = block_rows // 2
    seq_count, tp_count = lax.axis_size("seq"), lax.axis_size("tp")
    total = block_rows * seq_count
    reach = min(WINDOW, total // 2)
    back = min((reach - 2) // half + 1, 2 * seq_count - 1)

    def onward(hop):
        pairs = [(i, i + 1, 0) for i in range(hop - 1, seq_count - 1)]
        pairs = pairs + [(seq_count - 1, hop - 1, 0)] + [(i, i, 1) for i in range(hop - 1)]
        return [(a * tp_count + t, b * tp_count + (t ^ c)) for a, b, c in pairs for t in range(tp_count)]


    halves, normed, queries = [None] * (back + 2), [None, None], [None, None]
    halves[0], normed[1], weight, first_tokens, gain, cosine, sine, limits = second_half(
        tokens,
        norm_gain[None, :],
        key_weight,
        value_weight,
        rotation_tables(block_rows, seq_count),
        segments.reshape(-1, HEAD_DIM),
    )
    halves[1], normed[0] = first_half(first_tokens, gain, weight, cosine, sine)
    for distance in range(2, back + 2):
        halves[distance] = lax.ppermute(halves[distance - 2], ("seq", "tp"), onward(distance // 2))
    for part in (1, 0):
        queries[part] = query(part, normed[part], query_weight, cosine, sine)

    def swap(x, bit):
        return lax.ppermute(x, "tp", [(i, i ^ bit) for i in range(tp_count)])

    got, totals = {}, [None, None]
    for part in (1, 0):
        key_values = halves[1 - part : 1 - part + back + 1][::-1]
        if part == 1:
            before = attend(part, back, range(back - 2, back + 1), queries[part], limits, key_values, early=True)
            (mine,) = attend(part, back, range(back - 2), queries[part], limits, key_values, before=before)
        else:
            mine, *pair = attend(part, back, range(back + 1), queries[part], limits, key_values, pieces=2)
        if part == 1:
            x, y = swap(mine, 2), swap(mine, 4)
            has = {0: (mine,), 2: (x,), 4: (y,), 6: (swap(x, 4),)}
        else:
            y = [swap(a, 4) for a in pair]
            x = swap(mine, 2)
            has = {0: (mine,), 2: (x,), 4: tuple(y), 6: tuple(swap(a, 2) for a in y)}
        for bits in (0, 2, 4, 6):
            has[bits | 1] = tuple(swap(a, 1) for a in has[bits])
        got[part] = has
    for part in (1, 0):
        pieces = lambda *bits: [(b, got[part][b]) for b in bits]
        acc = None
        for bits in ((0, 1), (2, 3, 4, 5), (6, 7) if part == 1 else (6,)):
            acc = product(out_weight, pieces(*bits), acc)
        totals[part] = acc
    return store(out_weight, 7, [got[0][7]], totals)


def solution(mesh):
    return jax.shard_map(
        shards,
        mesh=mesh,
        in_specs=(P("seq", None), P(), P(None, "tp"), P(None, "tp"), P(None, "tp"), P(None, "tp"), P()),
        out_specs=P("seq", "tp"),
        check_vma=False,
    )
```
